256 devices in a mesh: blk: 64 (over z, x, core), head: 4 (over y).
Axes of the slice: x: 4, y: 4, z: 8, core: 2. Of those that a mesh axis runs over, the one named last changes fastest.
Arguments:
- layer_input: bfloat16 [32768, 5120], P(('blk', 'head')), may hold values from -0.125 to 0.125
- queries: bfloat16 [32768, 20, 128], P(('blk', 'head')), may hold values from -2 to 2
- key_vectors: bfloat16 [32768, 20, 128], P(('blk', 'head')), may hold values from -2 to 2
- value_vectors: bfloat16 [32768, 20, 128], P(('blk', 'head')), may hold values from -6 to 6
- out_grad: bfloat16 [32768, 20, 128], P(('blk', 'head')), may hold values from -24 to 24
- attn_out: bfloat16 [32768, 20, 128], P(('blk', 'head')), may hold values from -1.796875 to 1.796875
- log_sum: float32 [32768, 20], P(('blk', 'head')), may hold values from 5.5 to 8
- block_list: int32 [256, 8], replicated, may hold values from -1 to 255, as said below
Outputs:
- query_grad: bfloat16 [32768, 20, 128], P(('blk', 'head'))
- key_grad: bfloat16 [32768, 20, 128], P(('blk', 'head'))
- weight_grad: float32 [5120, 2560], P('blk', 'head')
The draws below stay inside these ranges and needn't reach their ends.
Inputs may be any that keep to these rules, and one draw needn't show every extreme that they name: `block_list`: row r lists distinct key blocks c (blocks of 128 tokens) with |c // 4 - r // 4| <= 1, block r among them, followed by -1 in the unused slots; some row uses all 8 slots.
All inputs are finite; a program needn't handle non-finite values.
Results may differ from the reference program's by a relative error of at most 0.0051.
Values may be sent and summed in bfloat16 or wider, within the bound.
A program may use at most 128 MiB of HBM per device.

```python
import jax
import jax.numpy as jnp
from jax import lax

D = 5120
H = 20
HD = 128
BLOCK = 128
KB = 8
BLOCKS_DEV = 4
TOKENS = 32768
N_BLK = 64


def draw_block_list(key, part):
    groups = N_BLK
    blocks = TOKENS // BLOCK
    split_keys = jax.random.split(jax.random.fold_in(key, 11), 5)
    device_ids = jnp.arange(groups)
    special = jax.random.randint(split_keys[2], (), 1, groups - 1)
    forced = (jnp.minimum(device_ids, groups - 1 - device_ids) <= 1) | (jnp.abs(device_ids - groups // 2) <= 1) | (device_ids == special)
    left_open = (jax.random.randint(split_keys[0], (groups,), 0, 4) > 0) | forced
    right_open = (jax.random.randint(split_keys[1], (groups,), 0, 4) > 0) | forced
    block_ids = jnp.arange(blocks)
    owner = block_ids // BLOCKS_DEV
    offset = owner[None, :] - owner[:, None]
    allowed = (offset == 0) | (offset == -1) & left_open[owner][:, None] | (offset == 1) & right_open[owner][:, None]
    distance = jnp.abs(block_ids[None, :] - block_ids[:, None])
    noise = jax.random.randint(split_keys[3], (blocks, blocks), 0, 4096)
    priority = noise - 1024 * distance + jnp.where(distance == 0, 1 << 20, 0) + jnp.where(distance == 1, 1 << 19, 0)
    priority = jnp.where(allowed, priority, -(1 << 30))
    ranked = jnp.argsort(-priority, axis=1, stable=True)[:, :KB]
    wanted = jax.random.randint(split_keys[4], (blocks,), 3, KB + 1)
    wanted = jnp.where(block_ids == special * BLOCKS_DEV, KB, wanted)
    wanted = jnp.minimum(wanted, jnp.sum(allowed.astype(jnp.int32), axis=1))
    slot_ids = jnp.arange(KB)
    return jnp.where(slot_ids[None, :] < wanted[:, None], ranked, -1).astype(jnp.int32)


def spiked(result, stream_key, source, target, shards_of, factor):
    owner, partner = [(jnp.arange(result.shape[dim]) // (result.shape[dim] // shards_of)).reshape([-1 if axis == dim else 1 for axis in range(result.ndim)]) for dim in (source, target)]
    chosen = jax.random.permutation(stream_key, shards_of)[partner]
    strong = (owner == chosen) | (owner == (partner + shards_of // 2) % shards_of)
    return jnp.where(strong, factor * result, result)


def steps_of(key, dims, cuts, least, largest):
    def one(dim, parts):
        draws = jax.random.uniform(jax.random.fold_in(jax.random.fold_in(key, 6), dim), (parts,), jnp.float32, least / len(cuts), largest / len(cuts))
        return jnp.repeat(jnp.exp(draws), dims[dim] // parts).reshape((-1,) + (1,) * (len(dims) - dim - 1))

    factor_of = one(*cuts[0])
    for cut in cuts[1:]:
        factor_of = factor_of * one(*cut)
    return factor_of


def centred(stream_key, extent, scale, most, cuts=(), kind=jnp.bfloat16):
    loudness = steps_of(stream_key, extent, cuts, -0.22, 0.18) if cuts else 1.0
    result = jax.random.normal(stream_key, extent, jnp.float32) * scale * loudness
    return jnp.minimum(jnp.maximum(result, -most), most).astype(kind)


def heavy_noise(own_key, dims, deviation, bound, pieces, heavy, kind=jnp.bfloat16):
    drawn = deviation * jax.random.normal(own_key, dims, jnp.float32)
    if pieces:
        drawn = drawn * steps_of(own_key, dims, pieces, -0.22, 0.18)
    return jnp.clip(spiked(drawn, jax.random.fold_in(own_key, 3), *heavy), -bound, bound).astype(kind)


def setup_inputs(seed: int = 0) -> dict:
    arg_keys = jax.random.split(jax.random.key(seed), 9)
    layer_input = heavy_noise(arg_keys[0], (TOKENS, D), TOKENS ** -0.5, 0.125, ((0, 256),), (0, 1, 256, 6.0))
    queries = jnp.clip(jax.random.uniform(arg_keys[1], (TOKENS, H, HD), jnp.float32, -2.0, 2.0) * steps_of(arg_keys[1], (TOKENS, H, HD), ((0, 256),), -0.4, 0.0), -2.0, 2.0).astype(jnp.bfloat16)
    key_vectors = jnp.clip(jax.random.uniform(arg_keys[2], (TOKENS, H, HD), jnp.float32, -2.0, 2.0) * steps_of(arg_keys[2], (TOKENS, H, HD), ((0, 256),), -0.4, 0.0), -2.0, 2.0).astype(jnp.bfloat16)
    value_vectors = centred(arg_keys[3], (TOKENS, H, HD), 1.0, 6.0, ((0, 256),))
    out_grad = centred(arg_keys[4], (TOKENS, H, HD), 4.0, 24.0, ((0, 256),))
    attn_out = centred(arg_keys[5], (TOKENS, H, HD), 0.3, 1.796875, ((0, 256),))
    log_sum = jnp.clip(5.5 + 2.5 * jax.random.uniform(arg_keys[6], (TOKENS, H), jnp.float32) ** steps_of(arg_keys[6], (TOKENS, H), ((0, 256),), -0.2, 0.2), 5.5, 8.0)
    block_list = draw_block_list(jax.random.fold_in(arg_keys[8], 71), 0)
    return dict(layer_input=layer_input, queries=queries, key_vectors=key_vectors, value_vectors=value_vectors, out_grad=out_grad, attn_out=attn_out, log_sum=log_sum, block_list=block_list)


def reference(layer_input, queries, key_vectors, value_vectors, out_grad, attn_out, log_sum, block_list):
    score_scale = HD ** -0.5
    row_delta = jnp.sum(out_grad.astype(jnp.float32) * attn_out.astype(jnp.float32), axis=2)
    block_total = TOKENS // BLOCK
    key_blocks = key_vectors.reshape(block_total, BLOCK, H, HD)
    value_blocks = value_vectors.reshape(block_total, BLOCK, H, HD)

    def one_block(carry, block_index):
        key_acc, value_acc = carry
        listed = block_list[block_index]
        present = (listed >= 0).astype(jnp.float32)
        chosen = jnp.where(listed >= 0, listed, 0).astype(jnp.int32)
        first_row = (block_index * BLOCK).astype(jnp.int32)
        query_rows = lax.dynamic_slice_in_dim(queries, first_row, BLOCK, 0).astype(jnp.float32)
        grad_rows = lax.dynamic_slice_in_dim(out_grad, first_row, BLOCK, 0).astype(jnp.float32)
        lse_rows = lax.dynamic_slice_in_dim(log_sum, first_row, BLOCK, 0)
        delta_rows = lax.dynamic_slice_in_dim(row_delta, first_row, BLOCK, 0)
        key_chosen = key_blocks[chosen].astype(jnp.float32)
        value_chosen = value_blocks[chosen].astype(jnp.float32)
        scores = jnp.einsum("qhd,jkhd->hqjk", query_rows, key_chosen) * score_scale
        weights = jnp.exp(scores - lse_rows.T[:, :, None, None]) * present[None, None, :, None]
        weights_b = lax.optimization_barrier(weights.astype(jnp.bfloat16)).astype(jnp.float32)
        dweights = jnp.einsum("qhd,jkhd->hqjk", grad_rows, value_chosen)
        dscores = weights * (dweights - delta_rows.T[:, :, None, None])
        dscores_b = lax.optimization_barrier(dscores.astype(jnp.bfloat16)).astype(jnp.float32)
        query_part = jnp.einsum("hqjk,jkhd->qhd", dscores_b, key_chosen) * score_scale
        key_part = jnp.einsum("hqjk,qhd->jkhd", dscores_b, query_rows) * score_scale
        value_part = jnp.einsum("hqjk,qhd->jkhd", weights_b, grad_rows)
        key_acc = key_acc.at[chosen].add(key_part)
        value_acc = value_acc.at[chosen].add(value_part)
        return (key_acc, value_acc), query_part

    zeros_acc = jnp.zeros((block_total, BLOCK, H, HD), jnp.float32)
    (key_acc, value_acc), query_parts = lax.scan(one_block, (zeros_acc, zeros_acc), jnp.arange(block_total, dtype=jnp.int32))
    query_grad = query_parts.reshape(TOKENS, H, HD).astype(jnp.bfloat16)
    key_grad = key_acc.reshape(TOKENS, H, HD).astype(jnp.bfloat16)
    value_grad = value_acc.reshape(TOKENS, H * HD).astype(jnp.bfloat16)
    weight_grad = jnp.dot(layer_input.T, value_grad, preferred_element_type=jnp.float32)
    return (query_grad, key_grad, weight_grad)
```

```python
import jax
import jax.numpy as jnp
from jax import lax
from jax.experimental import pallas as pl
from jax.experimental.pallas import tpu as pltpu
from jax.sharding import PartitionSpec as P

F32 = jnp.float32
BF16 = jnp.bfloat16
MESH = pl.DeviceIdType.MESH
SPAN = 512
TILE = 128
HEADS = 5
CHUNK = 256
HALF = 320
COLS = 640
N_BLK = 64
SCALE = 128 ** -0.5
FAR = 1e30
ORDER = (2, 1, 3, 0)


def push(src, dst, send, recv, **where):
    return pltpu.make_async_remote_copy(
        src_ref=src,
        dst_ref=dst,
        send_sem=send,
        recv_sem=recv,
        device_id=where,
        device_id_type=MESH,
    )


def meet(peers):
    barrier = pltpu.get_barrier_semaphore()
    for where in peers:
        pl.semaphore_signal(barrier, inc=1, device_id=where, device_id_type=MESH)
    pl.semaphore_wait(barrier, len(peers))


def rows(start):
    return pl.ds(pl.multiple_of(start, TILE), TILE)


def around(y):
    return lax.rem(y + 1, 4), lax.rem(y + 3, 4), lax.rem(y + 2, 4)


def entry_kernel(
    qg, kv_in, stat_in, lt, win, kv, stat, lt_x, relay,
    y_send, y_recv, s_send, s_recv, h_send, h_recv, t_send, t_recv, l_send, l_recv,
):
    b = lax.axis_index("blk")
    y = lax.axis_index("head")
    yr, yl, y2 = around(y)
    br, bl = lax.rem(b + 1, N_BLK), lax.rem(b + N_BLK - 1, N_BLK)
    core = lax.rem(b, 2)
    mate = b + 1 - 2 * core
    meet(
        [{"blk": b, "head": yr}, {"blk": b, "head": yl}, {"blk": b, "head": y2}]
        + [{"blk": br, "head": y}, {"blk": bl, "head": y}]
    )

    def mine(ref, to):
        return ref.at[:, pl.ds(to * HEADS, HEADS)]

    def one(ref, t, to):
        return ref.at[t, pl.ds(to * HEADS, HEADS)]

    def first(phase, src, dst, base):
        sends = []
        for i, (where, copy_from, copy_to) in enumerate(
            (
                (yr, one(src, 0, y2), relay.at[phase, 0]),
                (yl, one(src, 1, y2), relay.at[phase, 1]),
                (yr, mine(src, yr), dst.at[:, :, rows(base + y * TILE)]),
                (yl, mine(src, yl), dst.at[:, :, rows(base + y * TILE)]),
            )
        ):
            sends.append(
                push(copy_from, copy_to, y_send.at[phase, i], y_recv.at[phase, i], blk=b, head=where)
            )
            sends[-1].start()
        return sends

    def second(phase, sends, dst, base):
        sends[0].wait_recv()
        sends.append(
            push(
                relay.at[phase, 0], dst.at[0, :, rows(base + yl * TILE)],
                y_send.at[phase, 4], y_recv.at[phase, 4], blk=b, head=yr,
            )
        )
        sends[-1].start()
        sends[1].wait_recv()
        sends.append(
            push(
                relay.at[phase, 1], dst.at[1, :, rows(base + yr * TILE)],
                y_send.at[phase, 5], y_recv.at[phase, 5], blk=b, head=yl,
            )
        )
        sends[-1].start()

    stat_sends = []
    for i, where in enumerate((yr, yl, y2)):
        stat_sends.append(
            push(stat_in.at[where], stat.at[4 + y], s_send.at[i], s_recv.at[i], blk=b, head=where)
        )
        stat_sends[-1].start()
    queries = first(0, qg, win, SPAN)
    halo = []

    def pass_on(i, src, stat_src, owner):
        for j, (where, base, at) in enumerate(((br, 0, 0), (bl, 2 * SPAN, 8))):
            halo.append(
                push(
                    src, win.at[:, :, rows(base + owner * TILE)],
                    h_send.at[i, j], h_recv.at[i, j], blk=where, head=y,
                )
            )
            halo[-1].start()
            halo.append(
                push(
                    stat_src, stat.at[at + owner],
                    t_send.at[i, j], t_recv.at[i, j], blk=where, head=y,
                )
            )
            halo[-1].start()

    pass_on(0, mine(qg, y), stat_in.at[y], y)
    lt_copy = push(lt.at[:, 1 - core], lt_x, l_send, l_recv, blk=mate, head=y)
    lt_copy.start()
    for t in range(2):
        for h in range(HEADS):
            win[t, h, rows(SPAN + y * TILE)] = qg[t, y * HEADS + h]
            kv[t, h, rows(y * TILE)] = kv_in[t, y * HEADS + h]
    stat[4 + y] = stat_in[y]
    second(0, queries, win, SPAN)
    keys = first(1, kv_in, kv, 0)
    for i, owner in ((2, yl), (3, yr)):
        queries[i].wait_recv()
        stat_sends[i - 2].wait_recv()
        pass_on(i - 1, win.at[:, :, rows(SPAN + owner * TILE)], stat.at[4 + owner], owner)
    queries[4].wait_recv()
    queries[5].wait_recv()
    stat_sends[2].wait_recv()
    pass_on(3, win.at[:, :, rows(SPAN + y2 * TILE)], stat.at[4 + y2], y2)
    second(1, keys, kv, 0)
    for copy in keys[2:] + halo:
        copy.wait_recv()
    lt_copy.wait_recv()
    for copy in queries + keys + stat_sends + halo + [lt_copy]:
        copy.wait_send()


def dot(a, b, contract):
    return lax.dot_general(a, b, (contract, ((), ())), preferred_element_type=F32)


def main_kernel(
    win, kv, stat, far, lt, lt_x, grads, weight,
    gathered, dq, dk, dv, values, dq_out, dq_in, back, relay,
    x2_out, x2_in, xr_out, xr_in, xl_out, xl_in, total, z_out, z_in,
    own_sem, g_send, g_recv, v_send, v_recv, q_send, q_recv,
    x_send, x_recv, z_send, z_recv, b_send, b_recv,
):
    b = lax.axis_index("blk")
    y = lax.axis_index("head")
    yr, yl, y2 = around(y)
    br, bl = lax.rem(b + 1, N_BLK), lax.rem(b + N_BLK - 1, N_BLK)
    core = lax.rem(b, 2)
    mate = b + 1 - 2 * core
    x = lax.rem(b // 2, 4)
    z = b // 8
    xr = z * 8 + lax.rem(x + 1, 4) * 2 + core
    xl = z * 8 + lax.rem(x + 3, 4) * 2 + core

    def pair(owner):
        return pl.ds(pl.multiple_of(owner * 256, 256), 256)

    def lane(c):
        return pl.ds(pl.multiple_of(y * 256 + c * 128, 128), 128)

    own = []
    for i, dx in enumerate(ORDER):
        to = lax.rem(x + dx, 4)
        own.append(
            (
                pltpu.make_async_copy(lt.at[to, core], gathered.at[i, :, :, lane(core)], own_sem.at[i, 0]),
                pltpu.make_async_copy(lt_x.at[to], gathered.at[i, :, :, lane(1 - core)], own_sem.at[i, 1]),
            )
        )
        own[-1][0].start()
        own[-1][1].start()
    meet(
        [{"blk": b, "head": yr}, {"blk": b, "head": yl}, {"blk": b, "head": y2}]
        + [{"blk": br, "head": y}, {"blk": bl, "head": y}]
        + [{"blk": xr, "head": y}, {"blk": xl, "head": y}]
        + [{"blk": lax.rem(b + 8 * r, N_BLK), "head": y} for r in range(1, 8)]
    )
    gathers = {}

    def spread(i):
        own[i][0].wait()
        own[i][1].wait()
        for j, where in enumerate((yr, yl)):
            piece = gathered.at[i, :, :, pair(y)]
            gathers[i, j] = push(
                piece, piece, g_send.at[i, j], g_recv.at[i, j], blk=b, head=where
            )
            gathers[i, j].start()

    def forward(i):
        for j, (where, owner) in enumerate(((yr, yl), (yl, yr))):
            gathers[i, j].wait_recv()
            piece = gathered.at[i, j, :, pair(owner)]
            gathers[i, 2 + j] = push(
                piece, piece, g_send.at[i, 2 + j], g_recv.at[i, 2 + j], blk=b, head=where
            )
            gathers[i, 2 + j].start()

    def complete(i):
        gathers[i, 2].wait_recv()
        gathers[i, 3].wait_recv()

    def attend(step, carry):
        h = step // 6
        part = lax.rem(step, 6)
        at = pl.ds(pl.multiple_of(part * CHUNK, CHUNK), CHUNK)
        keys, vals = kv[0, h], kv[1, h]
        queries, grad = win[0, h, at], win[1, h, at]
        lo, hi = stat[2 * part, h], stat[2 * part + 1, h]
        far_lo, far_hi = far[2 * part], far[2 * part + 1]
        lse = jnp.concatenate([lo[0:1], hi[0:1]], axis=1)
        delta = jnp.concatenate([lo[1:2], hi[1:2]], axis=1)
        apart = jnp.concatenate([far_lo[0:4], far_hi[0:4]], axis=1) + lse
        scores = dot(keys, queries, ((1,), (1,))) * SCALE
        dweights = dot(vals, grad, ((1,), (1,)))
        weights = jnp.concatenate(
            [
                jnp.exp(scores[k * TILE : (k + 1) * TILE] - apart[k : k + 1])
                for k in range(4)
            ],
            axis=0,
        )
        dscores = (weights * (dweights - delta)).astype(BF16)
        weights = weights.astype(BF16)
        value_part = dot(weights, grad, ((1,), (0,)))
        key_part = dot(dscores, queries, ((1,), (0,)))
        dq[h, at] = dot(dscores, keys, ((0,), (0,))) * SCALE

        @pl.when(part == 0)
        def _():
            dv[h] = value_part
            dk[h] = key_part

        @pl.when(part != 0)
        def _():
            dv[h] += value_part
            dk[h] += key_part

        return carry

    spread(0)
    spread(1)
    lax.fori_loop(0, 18, attend, 0)
    forward(0)
    spread(2)
    lax.fori_loop(18, 30, attend, 0)
    forward(1)
    spread(3)

    for h in range(HEADS):
        cols = pl.ds(h * 128, 128)
        for k in range(4):
            values[k, core, :, cols] = dv[h, k * TILE : (k + 1) * TILE].astype(BF16)
    value_copy = push(
        values.at[:, core], values.at[:, core], v_send, v_recv, blk=mate, head=y
    )
    value_copy.start()
    for h in range(HEADS):
        dq_out[0, h] = dq[h, 0:SPAN].astype(BF16)
        dq_out[1, h] = dq[h, 2 * SPAN :].astype(BF16)
    dq_copies = []
    for j, where in enumerate((bl, br)):
        dq_copies.append(
            push(dq_out.at[j], dq_in.at[j], q_send.at[j], q_recv.at[j], blk=where, head=y)
        )
        dq_copies[-1].start()
    for h in range(HEADS):
        back[1, h] = (dk[h] * SCALE).astype(BF16)
    value_copy.wait_recv()

    def product(i, half):
        return dot(
            gathered[i, half], values[...].reshape(1024, COLS), ((1,), (0,))
        )

    complete(0)
    x_copies = []

    def x_push(i, src, dst, where):
        x_copies.append(push(src, dst, x_send.at[i], x_recv.at[i], blk=where, head=y))
        x_copies[-1].start()

    x2_out[0] = product(0, 0).astype(BF16)
    x_push(0, x2_out.at[0], x2_in.at[0], xr)
    x2_out[1] = product(0, 1).astype(BF16)
    x_push(1, x2_out.at[1], x2_in.at[1], xl)
    for copy in dq_copies:
        copy.wait_recv()
    for h in range(HEADS):
        back[0, h] = (
            dq[h, SPAN : 2 * SPAN] + dq_in[0, h].astype(F32) + dq_in[1, h].astype(F32)
        ).astype(BF16)
    forward(2)
    complete(1)
    first_half = product(1, 0)
    x_copies[0].wait_recv()
    xr_out[0] = (first_half + x2_in[0].astype(F32)).astype(BF16)
    x_push(2, xr_out.at[0], xr_in.at[0], xr)
    xr_out[1] = product(1, 1).astype(BF16)
    x_push(3, xr_out.at[1], xr_in.at[1], xr)
    forward(3)
    complete(2)
    xl_out[0] = product(2, 0).astype(BF16)
    x_push(4, xl_out.at[0], xl_in.at[0], xl)
    second_half = product(2, 1)
    x_copies[1].wait_recv()
    xl_out[1] = (second_half + x2_in[1].astype(F32)).astype(BF16)
    x_push(5, xl_out.at[1], xl_in.at[1], xl)

    back_copies = []
    for i, (where, copy_from, copy_to) in enumerate(
        (
            (yr, back.at[0, :, rows(y2 * TILE)], relay.at[0]),
            (yl, back.at[1, :, rows(y2 * TILE)], relay.at[1]),
            (yr, back.at[:, :, rows(yr * TILE)], grads.at[:, pl.ds(y * HEADS, HEADS)]),
            (yl, back.at[:, :, rows(yl * TILE)], grads.at[:, pl.ds(y * HEADS, HEADS)]),
        )
    ):
        back_copies.append(
            push(copy_from, copy_to, b_send.at[i], b_recv.at[i], blk=b, head=where)
        )
        back_copies[-1].start()
    for t in range(2):
        for h in range(HEADS):
            grads[t, y * HEADS + h] = back[t, h, rows(y * TILE)]
    complete(3)
    total[0] = product(3, 0)
    total[1] = product(3, 1)
    for j, (where, owner) in enumerate(((yr, yl), (yl, yr))):
        back_copies[j].wait_recv()
        back_copies.append(
            push(
                relay.at[j], grads.at[j, pl.ds(owner * HEADS, HEADS)],
                b_send.at[4 + j], b_recv.at[4 + j], blk=b, head=where,
            )
        )
        back_copies[-1].start()

    def sum_half(half):
        summed = total[half] + xr_in[half].astype(F32) + xl_in[half].astype(F32)
        total[half] = summed
        z_out[half] = summed.astype(BF16)

    def z_push(half):
        for k in range(4):
            to = 2 * k + half

            @pl.when(z != to)
            def _():
                push(
                    z_out.at[half, pl.ds(k * 80, 80)], z_in.at[lax.rem(to - z + 8, 8)],
                    z_send.at[lax.rem(to - z + 8, 8)], z_recv.at[lax.rem(to - z + 8, 8)],
                    blk=to * 8 + x * 2 + core, head=y,
                ).start()

    x_copies[2].wait_recv()
    x_copies[4].wait_recv()
    sum_half(0)
    z_push(0)
    x_copies[3].wait_recv()
    x_copies[5].wait_recv()
    sum_half(1)
    z_push(1)
    result = total[lax.rem(z, 2), pl.ds(pl.multiple_of((z // 2) * 80, 80), 80)]
    for r in range(1, 8):
        copy = push(
            z_out.at[0, pl.ds(0, 80)], z_in.at[r], z_send.at[r], z_recv.at[r],
            blk=lax.rem(b + 8 * r, N_BLK), head=y,
        )
        copy.wait_recv()
        result = result + z_in[r].astype(F32)
        copy.wait_send()
    weight[...] = result
    for copy in back_copies[2:]:
        copy.wait_recv()
    for copy in back_copies + x_copies + dq_copies + [value_copy] + list(gathers.values()):
        copy.wait_send()


VMEM_SPEC = pl.BlockSpec(memory_space=pltpu.VMEM)
ANY_SPEC = pl.BlockSpec(memory_space=pl.ANY)


def sems(*shape):
    return pltpu.SemaphoreType.DMA(shape) if shape else pltpu.SemaphoreType.DMA


def local(
    layer_input, queries, key_vectors, value_vectors, out_grad, attn_out, log_sum, block_list
):
    row_delta = jnp.sum(out_grad.astype(F32) * attn_out.astype(F32), axis=2)
    stats = jnp.stack((log_sum.T, row_delta.T), axis=1)
    stats = jnp.pad(stats, ((0, 0), (0, 6), (0, 0))).reshape(4, HEADS, 8, TILE)
    qg = jnp.stack((jnp.swapaxes(queries, 0, 1), jnp.swapaxes(out_grad, 0, 1)))
    kv = jnp.stack((jnp.swapaxes(key_vectors, 0, 1), jnp.swapaxes(value_vectors, 0, 1)))
    lt = layer_input.T.reshape(4, 2, 4, 2, 80, TILE)
    lt = jnp.transpose(lt, (2, 3, 1, 0, 4, 5)).reshape(4, 2, 2, HALF, TILE)

    first_block = lax.axis_index("blk") * 4
    padded = jnp.pad(block_list, ((4, 4), (0, 0)), constant_values=-1)
    lists = lax.dynamic_slice_in_dim(padded, first_block, 12, 0)
    own_ids = first_block + jnp.arange(8, dtype=jnp.int32)
    allowed = jnp.any(lists[:, None, :] == own_ids[None, :, None], axis=2)
    far = jnp.broadcast_to(jnp.where(allowed, 0.0, FAR)[:, :, None], (12, 8, TILE)).astype(F32)

    win, kv_all, stat, lt_x = pl.pallas_call(
        entry_kernel,
        out_shape=(
            jax.ShapeDtypeStruct((2, HEADS, 3 * SPAN, 128), BF16),
            jax.ShapeDtypeStruct((2, HEADS, SPAN, 128), BF16),
            jax.ShapeDtypeStruct((12, HEADS, 8, TILE), F32),
            jax.ShapeDtypeStruct((4, 2, HALF, TILE), BF16),
        ),
        in_specs=[VMEM_SPEC] * 3 + [ANY_SPEC],
        out_specs=[VMEM_SPEC] * 3 + [ANY_SPEC],
        scratch_shapes=[
            pltpu.VMEM((2, 2, HEADS, TILE, 128), BF16),
            sems(2, 6), sems(2, 6), sems(3), sems(3), sems(4, 2), sems(4, 2),
            sems(4, 2), sems(4, 2), sems(), sems(),
        ],
        compiler_params=pltpu.CompilerParams(
            collective_id=0, has_side_effects=True, vmem_limit_bytes=60 * 2**20
        ),
        name="entry",
    )(qg, kv, stats, lt)

    grads, weight = pl.pallas_call(
        main_kernel,
        out_shape=(
            jax.ShapeDtypeStruct((2, 20, TILE, 128), BF16),
            jax.ShapeDtypeStruct((80, COLS), F32),
        ),
        in_specs=[VMEM_SPEC] * 4 + [ANY_SPEC] * 2,
        out_specs=[VMEM_SPEC] * 2,
        scratch_shapes=[
            pltpu.VMEM((4, 2, HALF, 1024), BF16),
            pltpu.VMEM((HEADS, 3 * SPAN, 128), F32),
            pltpu.VMEM((HEADS, SPAN, 128), F32),
            pltpu.VMEM((HEADS, SPAN, 128), F32),
            pltpu.VMEM((4, 2, TILE, COLS), BF16),
            pltpu.VMEM((2, HEADS, SPAN, 128), BF16),
            pltpu.VMEM((2, HEADS, SPAN, 128), BF16),
            pltpu.VMEM((2, HEADS, SPAN, 128), BF16),
            pltpu.VMEM((2, HEADS, TILE, 128), BF16),
        ]
        + [pltpu.VMEM((2, HALF, COLS), BF16)] * 6
        + [
            pltpu.VMEM((2, HALF, COLS), F32),
            pltpu.VMEM((2, HALF, COLS), BF16),
            pltpu.VMEM((8, 80, COLS), BF16),
            sems(4, 2), sems(4, 4), sems(4, 4), sems(), sems(), sems(2), sems(2),
            sems(6), sems(6), sems(8), sems(8), sems(6), sems(6),
        ],
        compiler_params=pltpu.CompilerParams(
            collective_id=1, has_side_effects=True, vmem_limit_bytes=60 * 2**20
        ),
        name="main",
    )(win, kv_all, stat, far, lt, lt_x)
    return (jnp.swapaxes(grads[0], 0, 1), jnp.swapaxes(grads[1], 0, 1), weight)


def solution(mesh):
    both = ("blk", "head")
    rows3 = P(both, None, None)
    return jax.shard_map(
        local,
        mesh=mesh,
        in_specs=(P(both, None),) + (rows3,) * 5 + (P(both, None), P()),
        out_specs=(rows3, rows3, P("blk", "head")),
        check_vma=False,
    )
```

```python
import jax
import jax.numpy as jnp
from jax import lax
from jax.experimental import pallas as pl
from jax.experimental.pallas import tpu as pltpu
from jax.sharding import PartitionSpec as P

F32 = jnp.float32
BF16 = jnp.bfloat16
MESH = pl.DeviceIdType.MESH
SPAN = 512
TILE = 128
HEADS = 5
HALF = 320
COLS = 640
N_BLK = 64
SCALE = 128 ** -0.5
FAR = 1e30
ORDER = (2, 1, 3, 0)


def push(src, dst, send, recv, **where):
    return pltpu.make_async_remote_copy(
        src_ref=src,
        dst_ref=dst,
        send_sem=send,
        recv_sem=recv,
        device_id=where,
        device_id_type=MESH,
    )


def meet(peers):
    barrier = pltpu.get_barrier_semaphore()
    for where in peers:
        pl.semaphore_signal(barrier, inc=1, device_id=where, device_id_type=MESH)
    pl.semaphore_wait(barrier, len(peers))


def rows(start):
    return pl.ds(pl.multiple_of(start, TILE), TILE)


def around(y):
    return lax.rem(y + 1, 4), lax.rem(y + 3, 4), lax.rem(y + 2, 4)


def dot(a, b, contract):
    return lax.dot_general(a, b, (contract, ((), ())), preferred_element_type=F32)


def kernel(
    q_in, g_in, k_in, v_in, stat_in, far, lt, grads, weight,
    win, kv, stat, entry_relay, gathered, dq, dk, dv, values, dq_out, dq_in, back, relay,
    x2_out, x2_in, xr_out, xr_in, xl_out, xl_in, total, z_out, z_in,
    y_send, y_recv, s_send, s_recv, h_send, h_recv, t_send, t_recv, l_send, l_recv,
    own_sem, g_send, g_recv, v_send, v_recv, q_send, q_recv,
    x_send, x_recv, z_send, z_recv, b_send, b_recv,
):
    b = lax.axis_index("blk")
    y = lax.axis_index("head")
    yr, yl, y2 = around(y)
    br, bl = lax.rem(b + 1, N_BLK), lax.rem(b + N_BLK - 1, N_BLK)
    core = lax.rem(b, 2)
    mate = b + 1 - 2 * core
    x = lax.rem(b // 2, 4)
    z = b // 8
    xr = z * 8 + lax.rem(x + 1, 4) * 2 + core
    xl = z * 8 + lax.rem(x + 3, 4) * 2 + core

    def pair(owner):
        return pl.ds(pl.multiple_of(owner * 256, 256), 256)

    lane = pl.ds(pl.multiple_of(y * 256 + core * 128, 128), 128)
    turn = pl.ds(lax.rem(z + 3, 8), 8)
    own = []
    for i, dx in enumerate(ORDER):
        source = lt.at[lax.rem(x + dx, 4), core, turn]
        own.append(pltpu.make_async_copy(source, gathered.at[i, :, :, lane], own_sem.at[i]))
        own[-1].start()
    meet(
        [{"blk": b, "head": yr}, {"blk": b, "head": yl}, {"blk": b, "head": y2}]
        + [{"blk": br, "head": y}, {"blk": bl, "head": y}]
        + [{"blk": xr, "head": y}, {"blk": xl, "head": y}]
        + [{"blk": lax.rem(b + 8 * r, N_BLK), "head": y} for r in range(1, 8)]
    )

    def mine(ref, to):
        return ref.at[pl.ds(to * HEADS, HEADS)]

    def first(phase, srcs, dst, base):
        at = rows(base + y * TILE)
        plan = [
            (yr, mine(srcs[0], y2), entry_relay.at[phase, 0]),
            (yl, mine(srcs[1], y2), entry_relay.at[phase, 1]),
        ]
        for t in range(2):
            for where in (yr, yl):
                plan.append((where, mine(srcs[t], where), dst.at[t, :, at]))
        sends = []
        for i, (where, copy_from, copy_to) in enumerate(plan):
            sends.append(
                push(copy_from, copy_to, y_send.at[phase, i], y_recv.at[phase, i], blk=b, head=where)
            )
            sends[-1].start()
        return sends

    def second(phase, sends, dst, base):
        for j, (where, owner) in enumerate(((yr, yl), (yl, yr))):
            sends[j].wait_recv()
            sends.append(
                push(
                    entry_relay.at[phase, j], dst.at[j, :, rows(base + owner * TILE)],
                    y_send.at[phase, 6 + j], y_recv.at[phase, 6 + j], blk=b, head=where,
                )
            )
            sends[-1].start()

    stat_sends = []
    for i, where in enumerate((yr, yl, y2)):
        stat_sends.append(
            push(stat_in.at[where], stat.at[4 + y], s_send.at[i], s_recv.at[i], blk=b, head=where)
        )
        stat_sends[-1].start()
    keys = first(0, (k_in, v_in), kv, 0)
    halo = []

    def pass_on(i, srcs, stat_src, owner):
        for j, (where, base, at) in enumerate(((br, 0, 0), (bl, 2 * SPAN, 8))):
            for t in range(2):
                halo.append(
                    push(
                        srcs[t], win.at[t, :, rows(base + owner * TILE)],
                        h_send.at[i, j, t], h_recv.at[i, j, t], blk=where, head=y,
                    )
                )
                halo[-1].start()
            halo.append(
                push(
                    stat_src, stat.at[at + owner],
                    t_send.at[i, j], t_recv.at[i, j], blk=where, head=y,
                )
            )
            halo[-1].start()

    def landed(owner):
        return [win.at[t, :, rows(SPAN + owner * TILE)] for t in range(2)]

    pass_on(0, [mine(q_in, y), mine(g_in, y)], stat_in.at[y], y)
    swaps = []
    for i, dx in enumerate(ORDER):
        swaps.append(
            push(
                lt.at[lax.rem(x + dx, 4), 1 - core, turn], gathered.at[i, :, :, lane],
                l_send.at[i], l_recv.at[i], blk=mate, head=y,
            )
        )
        swaps[-1].start()
    for h in range(HEADS):
        for t, (near, key) in enumerate(((q_in, k_in), (g_in, v_in))):
            win[t, h, rows(SPAN + y * TILE)] = near[y * HEADS + h]
            kv[t, h, rows(y * TILE)] = key[y * HEADS + h]
    stat[4 + y] = stat_in[y]
    second(0, keys, kv, 0)
    queries = first(1, (q_in, g_in), win, SPAN)

    pieces = ((0, 0), (0, 1), (1, 0), (2, 0), (3, 0), (1, 1), (2, 1), (3, 1))
    gathers = {}
    for i in range(4):
        own[i].wait()

    def spread(p):
        i, half = pieces[p]
        if p in (0, 2, 3, 4):
            swaps[i].wait_recv()
        for j, where in enumerate((yr, yl)):
            piece = gathered.at[i, pl.ds(4 * half, 4), :, pair(y)]
            gathers[p, j] = push(
                piece, piece, g_send.at[p, j], g_recv.at[p, j], blk=b, head=where
            )
            gathers[p, j].start()

    def forward(p):
        i, half = pieces[p]
        for j, (where, owner) in enumerate(((yr, yl), (yl, yr))):
            gathers[p, j].wait_recv()
            piece = gathered.at[i, pl.ds(4 * half + 2 * j, 2), :, pair(owner)]
            gathers[p, 2 + j] = push(
                piece, piece, g_send.at[p, 2 + j], g_recv.at[p, 2 + j], blk=b, head=where
            )
            gathers[p, 2 + j].start()

    def product(p):
        i, half = pieces[p]
        gathers[p, 2].wait_recv()
        gathers[p, 3].wait_recv()
        left = gathered[i, 4 * half : 4 * half + 4].reshape(HALF, 1024)
        return dot(left, values[...].reshape(1024, COLS), ((1,), (0,)))

    def attend(owner, lead):
        spans = [rows(part * SPAN + owner * TILE) for part in range(3)]

        def one_head(h, carry):
            key, val = kv[0, h], kv[1, h]
            query = jnp.concatenate([win[0, h, at] for at in spans], axis=0)
            grad = jnp.concatenate([win[1, h, at] for at in spans], axis=0)
            tiles = [stat[4 * part + owner, h] for part in range(3)]
            lse = jnp.concatenate([tile[0:1] for tile in tiles], axis=1)
            delta = jnp.concatenate([tile[1:2] for tile in tiles], axis=1)
            apart = jnp.concatenate([far[4 * part + owner, 0:4] for part in range(3)], axis=1) + lse
            scores = dot(key, query, ((1,), (1,))) * SCALE
            dweights = dot(val, grad, ((1,), (1,)))
            weights = jnp.concatenate(
                [
                    jnp.exp(scores[k * TILE : (k + 1) * TILE] - apart[k : k + 1])
                    for k in range(4)
                ],
                axis=0,
            )
            dscores = (weights * (dweights - delta)).astype(BF16)
            weights = weights.astype(BF16)
            value_part = dot(weights, grad, ((1,), (0,)))
            key_part = dot(dscores, query, ((1,), (0,)))
            query_part = dot(dscores, key, ((0,), (0,))) * SCALE
            dq_out[0, h, rows(owner * TILE)] = query_part[:TILE].astype(BF16)
            dq[h, rows(owner * TILE)] = query_part[TILE : 2 * TILE]
            dq_out[1, h, rows(owner * TILE)] = query_part[2 * TILE :].astype(BF16)
            if lead:
                dv[h] = value_part
                dk[h] = key_part
            else:
                dv[h] += value_part
                dk[h] += key_part
            return carry

        lax.fori_loop(0, HEADS, one_head, 0)

    dq_copies = []

    def send_dq(i, owner):
        for j, where in enumerate((bl, br)):
            piece = (j, slice(None), rows(owner * TILE))
            dq_copies.append(
                push(
                    dq_out.at[piece], dq_in.at[piece],
                    q_send.at[i, j], q_recv.at[i, j], blk=where, head=y,
                )
            )
            dq_copies[-1].start()

    def halo_in(i):
        for copy in halo[6 * i : 6 * i + 6]:
            copy.wait_recv()

    for copy in keys[2:]:
        copy.wait_recv()
    second(1, queries, win, SPAN)
    spread(0)
    spread(1)
    spread(2)
    halo_in(0)
    attend(y, True)
    for i, owner in ((0, yl), (1, yr)):
        queries[2 + i].wait_recv()
        queries[4 + i].wait_recv()
        stat_sends[i].wait_recv()
        pass_on(1 + i, landed(owner), stat.at[4 + owner], owner)
    send_dq(0, y)
    halo_in(1)
    attend(yl, False)
    queries[6].wait_recv()
    queries[7].wait_recv()
    stat_sends[2].wait_recv()
    pass_on(3, landed(y2), stat.at[4 + y2], y2)
    send_dq(1, yl)
    halo_in(2)
    attend(yr, False)
    send_dq(2, yr)
    forward(0)
    spread(3)
    halo_in(3)
    attend(y2, False)

    for h in range(HEADS):
        cols = pl.ds(h * 128, 128)
        for k in range(4):
            values[k, core, :, cols] = dv[h, k * TILE : (k + 1) * TILE].astype(BF16)
    value_copy = push(
        values.at[:, core], values.at[:, core], v_send, v_recv, blk=mate, head=y
    )
    value_copy.start()
    send_dq(3, y2)
    forward(1)
    forward(2)
    spread(4)
    forward(3)
    spread(5)
    value_copy.wait_recv()
    x_copies = {}

    def x_push(name, i, q, src, dst, where):
        copy = push(src.at[q], dst.at[q], x_send.at[i, q], x_recv.at[i, q], blk=where, head=y)
        copy.start()
        x_copies[name, q] = copy

    def quarters(value):
        return ((0, value[:160]), (1, value[160:]))

    for q, part in quarters(product(0)):
        x2_out[q] = part.astype(BF16)
        x_push("far", 0, q, x2_out, x2_in, xr)
    for q, part in quarters(product(1)):
        x2_out[2 + q] = part.astype(BF16)
        x_push("far", 0, 2 + q, x2_out, x2_in, xl)
    for h in range(HEADS):
        back[1, h] = (dk[h] * SCALE).astype(BF16)
    forward(4)
    spread(6)
    for q, part in quarters(product(2)):
        x_copies["far", q].wait_recv()
        xr_out[q] = (part + x2_in[q].astype(F32)).astype(BF16)
        x_push("right", 1, q, xr_out, xr_in, xr)
    for q, part in quarters(product(3)):
        xl_out[q] = part.astype(BF16)
        x_push("left", 2, q, xl_out, xl_in, xl)
    forward(5)
    spread(7)
    total[0:HALF] = product(4)
    for q, part in quarters(product(5)):
        xr_out[2 + q] = part.astype(BF16)
        x_push("right", 1, 2 + q, xr_out, xr_in, xr)
    forward(6)
    for q, part in quarters(product(6)):
        x_copies["far", 2 + q].wait_recv()
        xl_out[2 + q] = (part + x2_in[2 + q].astype(F32)).astype(BF16)
        x_push("left", 2, 2 + q, xl_out, xl_in, xl)
    forward(7)

    for copy in dq_copies:
        copy.wait_recv()
    for h in range(HEADS):
        back[0, h] = (
            dq[h] + dq_in[0, h].astype(F32) + dq_in[1, h].astype(F32)
        ).astype(BF16)
    back_copies = []
    for i, (where, copy_from, copy_to) in enumerate(
        (
            (yr, back.at[0, :, rows(y2 * TILE)], relay.at[0]),
            (yl, back.at[1, :, rows(y2 * TILE)], relay.at[1]),
            (yr, back.at[:, :, rows(yr * TILE)], grads.at[:, pl.ds(y * HEADS, HEADS)]),
            (yl, back.at[:, :, rows(yl * TILE)], grads.at[:, pl.ds(y * HEADS, HEADS)]),
        )
    ):
        back_copies.append(
            push(copy_from, copy_to, b_send.at[i], b_recv.at[i], blk=b, head=where)
        )
        back_copies[-1].start()
    for t in range(2):
        for h in range(HEADS):
            grads[t, y * HEADS + h] = back[t, h, rows(y * TILE)]

    z_copies = {}

    def reduce_quarter(q):
        x_copies["right", q].wait_recv()
        x_copies["left", q].wait_recv()
        at = pl.ds(160 * q, 160)
        summed = total[at] + xr_in[q].astype(F32) + xl_in[q].astype(F32)
        for k in range(2):
            r = (3 + 2 * q + k) % 8
            part = summed[80 * k : 80 * k + 80]
            if r == 0:
                weight[...] = part
                continue
            z_out[r] = part.astype(BF16)
            z_copies[r] = push(
                z_out.at[r], z_in.at[r], z_send.at[r], z_recv.at[r],
                blk=lax.rem(b + 8 * r, N_BLK), head=y,
            )
            z_copies[r].start()

    reduce_quarter(0)
    reduce_quarter(1)
    total[HALF : 2 * HALF] = product(7)
    reduce_quarter(2)
    for j, (where, owner) in enumerate(((yr, yl), (yl, yr))):
        back_copies[j].wait_recv()
        back_copies.append(
            push(
                relay.at[j], grads.at[j, pl.ds(owner * HEADS, HEADS)],
                b_send.at[4 + j], b_recv.at[4 + j], blk=b, head=where,
            )
        )
        back_copies[-1].start()

    reduce_quarter(3)
    result = weight[...]
    for r in (3, 4, 5, 6, 7, 1, 2):
        z_copies[r].wait_recv()
        result = result + z_in[r].astype(F32)
    weight[...] = result
    for copy in back_copies[2:]:
        copy.wait_recv()
    copies = queries + keys + stat_sends + halo + swaps + list(gathers.values())
    copies += list(x_copies.values()) + list(z_copies.values())
    for copy in copies + [value_copy] + dq_copies + back_copies:
        copy.wait_send()


VMEM_SPEC = pl.BlockSpec(memory_space=pltpu.VMEM)
ANY_SPEC = pl.BlockSpec(memory_space=pl.ANY)


def sems(*shape):
    return pltpu.SemaphoreType.DMA(shape) if shape else pltpu.SemaphoreType.DMA


def local(
    layer_input, queries, key_vectors, value_vectors, out_grad, attn_out, log_sum, block_list
):
    row_delta = jnp.sum(out_grad.astype(F32) * attn_out.astype(F32), axis=2)
    stats = jnp.stack((log_sum.T, row_delta.T), axis=1)
    stats = jnp.pad(stats, ((0, 0), (0, 6), (0, 0))).reshape(4, HEADS, 8, TILE)
    by_head = [
        jnp.swapaxes(array, 0, 1) for array in (queries, out_grad, key_vectors, value_vectors)
    ]
    lt = jnp.transpose(layer_input.T.reshape(8, 4, 2, 80, TILE), (1, 2, 0, 3, 4))
    lt = jnp.concatenate((lt, lt), axis=2)

    first_block = lax.axis_index("blk") * 4
    padded = jnp.pad(block_list, ((4, 4), (0, 0)), constant_values=-1)
    lists = lax.dynamic_slice_in_dim(padded, first_block, 12, 0)
    own_ids = first_block + jnp.arange(8, dtype=jnp.int32)
    allowed = jnp.any(lists[:, None, :] == own_ids[None, :, None], axis=2)
    far = jnp.broadcast_to(jnp.where(allowed, 0.0, FAR)[:, :, None], (12, 8, TILE)).astype(F32)

    grads, weight = pl.pallas_call(
        kernel,
        out_shape=(
            jax.ShapeDtypeStruct((2, 20, TILE, 128), BF16),
            jax.ShapeDtypeStruct((80, COLS), F32),
        ),
        in_specs=[VMEM_SPEC] * 6 + [ANY_SPEC],
        out_specs=[VMEM_SPEC] * 2,
        scratch_shapes=[
            pltpu.VMEM((2, HEADS, 3 * SPAN, 128), BF16),
            pltpu.VMEM((2, HEADS, SPAN, 128), BF16),
            pltpu.VMEM((12, HEADS, 8, TILE), F32),
            pltpu.VMEM((2, 2, HEADS, TILE, 128), BF16),
            pltpu.VMEM((4, 8, 80, 1024), BF16),
            pltpu.VMEM((HEADS, SPAN, 128), F32),
            pltpu.VMEM((HEADS, SPAN, 128), F32),
            pltpu.VMEM((HEADS, SPAN, 128), F32),
            pltpu.VMEM((4, 2, TILE, COLS), BF16),
            pltpu.VMEM((2, HEADS, SPAN, 128), BF16),
            pltpu.VMEM((2, HEADS, SPAN, 128), BF16),
            pltpu.VMEM((2, HEADS, SPAN, 128), BF16),
            pltpu.VMEM((2, HEADS, TILE, 128), BF16),
        ]
        + [pltpu.VMEM((4, 160, COLS), BF16)] * 6
        + [
            pltpu.VMEM((2 * HALF, COLS), F32),
            pltpu.VMEM((8, 80, COLS), BF16),
            pltpu.VMEM((8, 80, COLS), BF16),
            sems(2, 8), sems(2, 8), sems(3), sems(3), sems(4, 2, 2), sems(4, 2, 2),
            sems(4, 2), sems(4, 2), sems(4), sems(4),
            sems(4), sems(8, 4), sems(8, 4), sems(), sems(), sems(4, 2), sems(4, 2),
            sems(3, 4), sems(3, 4), sems(8), sems(8), sems(6), sems(6),
        ],
        compiler_params=pltpu.CompilerParams(
            collective_id=0, has_side_effects=True, vmem_limit_bytes=60 * 2**20
        ),
        name="layer",
    )(*by_head, stats, far, lt)
    return (jnp.swapaxes(grads[0], 0, 1), jnp.swapaxes(grads[1], 0, 1), weight)


def solution(mesh):
    both = ("blk", "head")
    rows3 = P(both, None, None)
    return jax.shard_map(
        local,
        mesh=mesh,
        in_specs=(P(both, None),) + (rows3,) * 5 + (P(both, None), P()),
        out_specs=(rows3, rows3, P("blk", "head")),
        check_vma=False,
    )
```

```python
import jax
import jax.numpy as jnp
from jax import lax
from jax.experimental import pallas as pl
from jax.experimental.pallas import tpu as pltpu
from jax.sharding import PartitionSpec as P

F32 = jnp.float32
BF16 = jnp.bfloat16
MESH = pl.DeviceIdType.MESH
SPAN = 512
TILE = 128
HEADS = 5
HALF = 320
COLS = 640
N_BLK = 64
SCALE = 128 ** -0.5
FAR = 1e30
ORDER = (2, 1, 3, 0)


def push(src, dst, send, recv, **where):
    return pltpu.make_async_remote_copy(
        src_ref=src,
        dst_ref=dst,
        send_sem=send,
        recv_sem=recv,
        device_id=where,
        device_id_type=MESH,
    )


def meet(peers):
    barrier = pltpu.get_barrier_semaphore()
    for where in peers:
        pl.semaphore_signal(barrier, inc=1, device_id=where, device_id_type=MESH)
    pl.semaphore_wait(barrier, len(peers))


def rows(start):
    return pl.ds(pl.multiple_of(start, TILE), TILE)


def around(y):
    return lax.rem(y + 1, 4), lax.rem(y + 3, 4), lax.rem(y + 2, 4)


def dot(a, b, contract):
    return lax.dot_general(a, b, (contract, ((), ())), preferred_element_type=F32)


def kernel(
    q_in, g_in, k_in, v_in, lse_in, a_hbm, l_hbm, listed, query_out, key_out, weight,
    a_in, l_in, lt, stat_in, far,
    win, kv, stat, entry_relay, gathered, dq, dk, dv, values, dq_out, dq_in, back, relay,
    x2_out, x2_in, xr_out, xr_in, xl_out, xl_in, total, z_out, z_in,
    y_send, y_recv, s_send, s_recv, h_send, h_recv, t_send, t_recv, l_send, l_recv,
    own_sem, g_send, g_recv, v_send, v_recv, q_send, q_recv,
    x_send, x_recv, z_send, z_recv, b_send, b_recv,
):
    b = lax.axis_index("blk")
    y = lax.axis_index("head")
    yr, yl, y2 = around(y)
    br, bl = lax.rem(b + 1, N_BLK), lax.rem(b + N_BLK - 1, N_BLK)
    core = lax.rem(b, 2)
    mate = b + 1 - 2 * core
    x = lax.rem(b // 2, 4)
    z = b // 8
    xr = z * 8 + lax.rem(x + 1, 4) * 2 + core
    xl = z * 8 + lax.rem(x + 3, 4) * 2 + core

    def pair(owner):
        return pl.ds(pl.multiple_of(owner * 256, 256), 256)

    lane = pl.ds(pl.multiple_of(y * 256 + core * 128, 128), 128)
    grads = (query_out, key_out)
    a_load = pltpu.make_async_copy(a_hbm, a_in, own_sem.at[0])
    l_load = pltpu.make_async_copy(l_hbm, l_in, own_sem.at[1])
    a_load.start()
    l_load.start()
    meet(
        [{"blk": b, "head": yr}, {"blk": b, "head": yl}, {"blk": b, "head": y2}]
        + [{"blk": br, "head": y}, {"blk": bl, "head": y}]
        + [{"blk": xr, "head": y}, {"blk": xl, "head": y}]
        + [{"blk": lax.rem(b + 8 * r, N_BLK), "head": y} for r in range(1, 8)]
    )

    def mine(ref, to):
        return ref.at[pl.ds(to * HEADS, HEADS)]

    def first(phase, srcs, dst, base):
        at = rows(base + y * TILE)
        plan = [
            (yr, mine(srcs[0], y2), entry_relay.at[phase, 0]),
            (yl, mine(srcs[1], y2), entry_relay.at[phase, 1]),
        ]
        for t in range(2):
            for where in (yr, yl):
                plan.append((where, mine(srcs[t], where), dst.at[t, :, at]))
        sends = []
        for i, (where, copy_from, copy_to) in enumerate(plan):
            sends.append(
                push(copy_from, copy_to, y_send.at[phase, i], y_recv.at[phase, i], blk=b, head=where)
            )
            sends[-1].start()
        return sends

    def second(phase, sends, dst, base):
        for j, (where, owner) in enumerate(((yr, yl), (yl, yr))):
            sends[j].wait_recv()
            sends.append(
                push(
                    entry_relay.at[phase, j], dst.at[j, :, rows(base + owner * TILE)],
                    y_send.at[phase, 6 + j], y_recv.at[phase, 6 + j], blk=b, head=where,
                )
            )
            sends[-1].start()

    keys = first(0, (k_in, v_in), kv, 0)
    halo = []
    halo_stat = {}

    def pass_on(i, srcs, stat_src, owner):
        for j, (where, base, at) in enumerate(((br, 0, 0), (bl, 2 * SPAN, 8))):
            for t in range(2):
                halo.append(
                    push(
                        srcs[t], win.at[t, :, rows(base + owner * TILE)],
                        h_send.at[i, j, t], h_recv.at[i, j, t], blk=where, head=y,
                    )
                )
                halo[-1].start()
            if stat_src is not None:
                stat_on(i, j, where, stat_src, at + owner)

    def stat_on(i, j, where, stat_src, at):
        halo_stat[i, j] = push(
            stat_src, stat.at[at], t_send.at[i, j], t_recv.at[i, j], blk=where, head=y
        )
        halo_stat[i, j].start()

    def landed(owner):
        return [win.at[t, :, rows(SPAN + owner * TILE)] for t in range(2)]

    pass_on(0, [mine(q_in, y), mine(g_in, y)], None, y)
    for h in range(HEADS):
        for t, (near, key) in enumerate(((q_in, k_in), (g_in, v_in))):
            win[t, h, rows(SPAN + y * TILE)] = near[y * HEADS + h]
            kv[t, h, rows(y * TILE)] = key[y * HEADS + h]
    a_load.wait()

    def head_stat(h, carry):
        product = g_in[h].astype(F32) * a_in[h].astype(F32)
        delta = jnp.sum(product.T, axis=0, keepdims=True)
        lse = lse_in[pl.ds(h, 1), :]
        tile = jnp.concatenate([lse, delta, jnp.zeros((6, TILE), F32)], axis=0)
        stat_in[h // HEADS, lax.rem(h, HEADS)] = tile
        return carry

    lax.fori_loop(0, 4 * HEADS, head_stat, 0)
    second(0, keys, kv, 0)
    queries = first(1, (q_in, g_in), win, SPAN)
    stat[4 + y] = stat_in[y]
    stat_sends = []
    for i, where in enumerate((yr, yl, y2)):
        stat_sends.append(
            push(stat_in.at[where], stat.at[4 + y], s_send.at[i], s_recv.at[i], blk=b, head=where)
        )
        stat_sends[-1].start()
    for j, (where, at) in enumerate(((br, 0), (bl, 8))):
        stat_on(0, j, where, stat_in.at[y], at + y)

    l_load.wait()
    for j in range(40):
        lt[128 * j : 128 * j + 128] = l_in[:, 128 * j : 128 * j + 128].T

    def rows_of(dx, k, c):
        to = (lax.rem(z + 3 + k, 8) * 4 + lax.rem(x + dx, 4)) * 2 + c
        return pl.ds(pl.multiple_of(to * 80, 16), 80)

    for i, dx in enumerate(ORDER):
        for k in range(8):
            gathered[i, k, :, lane] = lt[rows_of(dx, k, core)]
    swaps = []
    for i, dx in enumerate(ORDER):
        for k in range(8):
            swaps.append(
                push(
                    lt.at[rows_of(dx, k, 1 - core)], gathered.at[i, k, :, lane],
                    l_send.at[i, k], l_recv.at[i, k], blk=mate, head=y,
                )
            )
            swaps[-1].start()
    for row in range(12):
        block = b * 4 + (row - 4)
        inside = (block >= 0) & (block < 4 * N_BLK)
        at = jnp.clip(block, 0, 4 * N_BLK - 1)
        entries = [listed[slot, at] for slot in range(8)]
        lines = []
        for k in range(4):
            found = entries[0] == b * 4 + k
            for entry in entries[1:]:
                found = found | (entry == b * 4 + k)
            gap = jnp.where(found & inside, jnp.float32(0.0), jnp.float32(FAR))
            lines.append(jnp.full((1, TILE), gap, F32))
        far[row] = jnp.concatenate(lines + lines, axis=0)

    pieces = ((0, 0), (0, 1), (1, 0), (2, 0), (3, 0), (1, 1), (2, 1), (3, 1))
    gathers = {}

    def spread(p):
        i, half = pieces[p]
        if p in (0, 2, 3, 4):
            for copy in swaps[8 * i : 8 * i + 8]:
                copy.wait_recv()
        for j, where in enumerate((yr, yl)):
            piece = gathered.at[i, pl.ds(4 * half, 4), :, pair(y)]
            gathers[p, j] = push(
                piece, piece, g_send.at[p, j], g_recv.at[p, j], blk=b, head=where
            )
            gathers[p, j].start()

    def forward(p):
        i, half = pieces[p]
        for j, (where, owner) in enumerate(((yr, yl), (yl, yr))):
            gathers[p, j].wait_recv()
            piece = gathered.at[i, pl.ds(4 * half + 2 * j, 2), :, pair(owner)]
            gathers[p, 2 + j] = push(
                piece, piece, g_send.at[p, 2 + j], g_recv.at[p, 2 + j], blk=b, head=where
            )
            gathers[p, 2 + j].start()

    def product(p):
        i, half = pieces[p]
        gathers[p, 2].wait_recv()
        gathers[p, 3].wait_recv()
        left = gathered[i, 4 * half : 4 * half + 4].reshape(HALF, 1024)
        return dot(left, values[...].reshape(1024, COLS), ((1,), (0,)))

    def attend(owner, lead):
        spans = [rows(part * SPAN + owner * TILE) for part in range(3)]

        def one_head(h, carry):
            key, val = kv[0, h], kv[1, h]
            query = jnp.concatenate([win[0, h, at] for at in spans], axis=0)
            grad = jnp.concatenate([win[1, h, at] for at in spans], axis=0)
            tiles = [stat[4 * part + owner, h] for part in range(3)]
            lse = jnp.concatenate([tile[0:1] for tile in tiles], axis=1)
            delta = jnp.concatenate([tile[1:2] for tile in tiles], axis=1)
            apart = jnp.concatenate([far[4 * part + owner, 0:4] for part in range(3)], axis=1) + lse
            scores = dot(key, query, ((1,), (1,))) * SCALE
            dweights = dot(val, grad, ((1,), (1,)))
            weights = jnp.concatenate(
                [
                    jnp.exp(scores[k * TILE : (k + 1) * TILE] - apart[k : k + 1])
                    for k in range(4)
                ],
                axis=0,
            )
            dscores = (weights * (dweights - delta)).astype(BF16)
            weights = weights.astype(BF16)
            value_part = dot(weights, grad, ((1,), (0,)))
            key_part = dot(dscores, query, ((1,), (0,)))
            query_part = dot(dscores, key, ((0,), (0,))) * SCALE
            dq_out[0, h, rows(owner * TILE)] = query_part[:TILE].astype(BF16)
            dq[h, rows(owner * TILE)] = query_part[TILE : 2 * TILE]
            dq_out[1, h, rows(owner * TILE)] = query_part[2 * TILE :].astype(BF16)
            if lead:
                dv[h] = value_part
                dk[h] = key_part
            else:
                dv[h] += value_part
                dk[h] += key_part
            return carry

        lax.fori_loop(0, HEADS, one_head, 0)

    dq_copies = []

    def send_dq(i, owner):
        for j, where in enumerate((bl, br)):
            piece = (j, slice(None), rows(owner * TILE))
            dq_copies.append(
                push(
                    dq_out.at[piece], dq_in.at[piece],
                    q_send.at[i, j], q_recv.at[i, j], blk=where, head=y,
                )
            )
            dq_copies[-1].start()

    def halo_in(i):
        for copy in halo[4 * i : 4 * i + 4] + [halo_stat[i, 0], halo_stat[i, 1]]:
            copy.wait_recv()

    for copy in keys[2:]:
        copy.wait_recv()
    second(1, queries, win, SPAN)
    spread(0)
    spread(1)
    spread(2)
    halo_in(0)
    attend(y, True)
    for i, owner in ((0, yl), (1, yr)):
        queries[2 + i].wait_recv()
        queries[4 + i].wait_recv()
        stat_sends[i].wait_recv()
        pass_on(1 + i, landed(owner), stat.at[4 + owner], owner)
    send_dq(0, y)
    halo_in(1)
    attend(yl, False)
    queries[6].wait_recv()
    queries[7].wait_recv()
    stat_sends[2].wait_recv()
    pass_on(3, landed(y2), stat.at[4 + y2], y2)
    send_dq(1, yl)
    halo_in(2)
    attend(yr, False)
    send_dq(2, yr)
    forward(0)
    spread(3)
    halo_in(3)
    attend(y2, False)

    for h in range(HEADS):
        cols = pl.ds(h * 128, 128)
        for k in range(4):
            values[k, core, :, cols] = dv[h, k * TILE : (k + 1) * TILE].astype(BF16)
    value_copy = push(
        values.at[:, core], values.at[:, core], v_send, v_recv, blk=mate, head=y
    )
    value_copy.start()
    send_dq(3, y2)
    forward(1)
    forward(2)
    spread(4)
    forward(3)
    spread(5)
    value_copy.wait_recv()
    x_copies = {}

    def x_push(name, i, q, src, dst, where):
        copy = push(src.at[q], dst.at[q], x_send.at[i, q], x_recv.at[i, q], blk=where, head=y)
        copy.start()
        x_copies[name, q] = copy

    def quarters(value):
        return ((0, value[:160]), (1, value[160:]))

    for q, part in quarters(product(0)):
        x2_out[q] = part.astype(BF16)
        x_push("far", 0, q, x2_out, x2_in, xr)
    for q, part in quarters(product(1)):
        x2_out[2 + q] = part.astype(BF16)
        x_push("far", 0, 2 + q, x2_out, x2_in, xl)
    for h in range(HEADS):
        back[1, h] = (dk[h] * SCALE).astype(BF16)
    forward(4)
    spread(6)
    for q, part in quarters(product(2)):
        x_copies["far", q].wait_recv()
        xr_out[q] = (part + x2_in[q].astype(F32)).astype(BF16)
        x_push("right", 1, q, xr_out, xr_in, xr)
    for q, part in quarters(product(3)):
        xl_out[q] = part.astype(BF16)
        x_push("left", 2, q, xl_out, xl_in, xl)
    forward(5)
    spread(7)
    total[0:HALF] = product(4)
    for q, part in quarters(product(5)):
        xr_out[2 + q] = part.astype(BF16)
        x_push("right", 1, 2 + q, xr_out, xr_in, xr)
    forward(6)
    for q, part in quarters(product(6)):
        x_copies["far", 2 + q].wait_recv()
        xl_out[2 + q] = (part + x2_in[2 + q].astype(F32)).astype(BF16)
        x_push("left", 2, 2 + q, xl_out, xl_in, xl)
    forward(7)

    for copy in dq_copies:
        copy.wait_recv()
    for h in range(HEADS):
        back[0, h] = (
            dq[h] + dq_in[0, h].astype(F32) + dq_in[1, h].astype(F32)
        ).astype(BF16)
    plan = [
        (yr, back.at[0, :, rows(y2 * TILE)], relay.at[0]),
        (yl, back.at[1, :, rows(y2 * TILE)], relay.at[1]),
    ]
    for t in range(2):
        for where in (yr, yl):
            plan.append((where, back.at[t, :, rows(where * TILE)], mine(grads[t], y)))
    back_copies = []
    for i, (where, copy_from, copy_to) in enumerate(plan):
        back_copies.append(
            push(copy_from, copy_to, b_send.at[i], b_recv.at[i], blk=b, head=where)
        )
        back_copies[-1].start()
    for t in range(2):
        for h in range(HEADS):
            grads[t][y * HEADS + h] = back[t, h, rows(y * TILE)]

    z_copies = {}

    def reduce_quarter(q):
        x_copies["right", q].wait_recv()
        x_copies["left", q].wait_recv()
        at = pl.ds(160 * q, 160)
        summed = total[at] + xr_in[q].astype(F32) + xl_in[q].astype(F32)
        for k in range(2):
            r = (3 + 2 * q + k) % 8
            part = summed[80 * k : 80 * k + 80]
            if r == 0:
                weight[...] = part
                continue
            z_out[r] = part.astype(BF16)
            z_copies[r] = push(
                z_out.at[r], z_in.at[r], z_send.at[r], z_recv.at[r],
                blk=lax.rem(b + 8 * r, N_BLK), head=y,
            )
            z_copies[r].start()

    reduce_quarter(0)
    reduce_quarter(1)
    total[HALF : 2 * HALF] = product(7)
    reduce_quarter(2)
    for j, (where, owner) in enumerate(((yr, yl), (yl, yr))):
        back_copies[j].wait_recv()
        back_copies.append(
            push(
                relay.at[j], mine(grads[j], owner),
                b_send.at[6 + j], b_recv.at[6 + j], blk=b, head=where,
            )
        )
        back_copies[-1].start()

    reduce_quarter(3)
    result = weight[...]
    for r in (3, 4, 5, 6, 7, 1, 2):
        z_copies[r].wait_recv()
        result = result + z_in[r].astype(F32)
    weight[...] = result
    for copy in back_copies[2:]:
        copy.wait_recv()
    copies = queries + keys + stat_sends + halo + swaps + list(gathers.values())
    copies += list(x_copies.values()) + list(z_copies.values()) + list(halo_stat.values())
    for copy in copies + [value_copy] + dq_copies + back_copies:
        copy.wait_send()


VMEM_SPEC = pl.BlockSpec(memory_space=pltpu.VMEM)
ANY_SPEC = pl.BlockSpec(memory_space=pl.ANY)


def sems(*shape):
    return pltpu.SemaphoreType.DMA(shape) if shape else pltpu.SemaphoreType.DMA


def local(
    layer_input, queries, key_vectors, value_vectors, out_grad, attn_out, log_sum, block_list
):
    by_head = [
        jnp.swapaxes(array, 0, 1)
        for array in (queries, out_grad, key_vectors, value_vectors, attn_out)
    ]
    query_grad, key_grad, weight_grad = pl.pallas_call(
        kernel,
        out_shape=(
            jax.ShapeDtypeStruct((20, TILE, 128), BF16),
            jax.ShapeDtypeStruct((20, TILE, 128), BF16),
            jax.ShapeDtypeStruct((80, COLS), F32),
        ),
        in_specs=[VMEM_SPEC] * 5 + [ANY_SPEC] * 2 + [pl.BlockSpec(memory_space=pltpu.SMEM)],
        out_specs=[VMEM_SPEC] * 3,
        scratch_shapes=[
            pltpu.VMEM((20, TILE, 128), BF16),
            pltpu.VMEM((TILE, 5120), BF16),
            pltpu.VMEM((5120, TILE), BF16),
            pltpu.VMEM((4, HEADS, 8, TILE), F32),
            pltpu.VMEM((12, 8, TILE), F32),
            pltpu.VMEM((2, HEADS, 3 * SPAN, 128), BF16),
            pltpu.VMEM((2, HEADS, SPAN, 128), BF16),
            pltpu.VMEM((12, HEADS, 8, TILE), F32),
            pltpu.VMEM((2, 2, HEADS, TILE, 128), BF16),
            pltpu.VMEM((4, 8, 80, 1024), BF16),
            pltpu.VMEM((HEADS, SPAN, 128), F32),
            pltpu.VMEM((HEADS, SPAN, 128), F32),
            pltpu.VMEM((HEADS, SPAN, 128), F32),
            pltpu.VMEM((4, 2, TILE, COLS), BF16),
            pltpu.VMEM((2, HEADS, SPAN, 128), BF16),
            pltpu.VMEM((2, HEADS, SPAN, 128), BF16),
            pltpu.VMEM((2, HEADS, SPAN, 128), BF16),
            pltpu.VMEM((2, HEADS, TILE, 128), BF16),
        ]
        + [pltpu.VMEM((4, 160, COLS), BF16)] * 6
        + [
            pltpu.VMEM((2 * HALF, COLS), F32),
            pltpu.VMEM((8, 80, COLS), BF16),
            pltpu.VMEM((8, 80, COLS), BF16),
            sems(2, 8), sems(2, 8), sems(3), sems(3), sems(4, 2, 2), sems(4, 2, 2),
            sems(4, 2), sems(4, 2), sems(4, 8), sems(4, 8),
            sems(2), sems(8, 4), sems(8, 4), sems(), sems(), sems(4, 2), sems(4, 2),
            sems(3, 4), sems(3, 4), sems(8), sems(8), sems(8), sems(8),
        ],
        compiler_params=pltpu.CompilerParams(
            collective_id=0, has_side_effects=True, vmem_limit_bytes=60 * 2**20
        ),
        name="layer",
    )(*by_head[:4], log_sum.T, by_head[4], layer_input, block_list.T)
    return (jnp.swapaxes(query_grad, 0, 1), jnp.swapaxes(key_grad, 0, 1), weight_grad)


def solution(mesh):
    both = ("blk", "head")
    rows3 = P(both, None, None)
    return jax.shard_map(
        local,
        mesh=mesh,
        in_specs=(P(both, None),) + (rows3,) * 5 + (P(both, None), P()),
        out_specs=(rows3, rows3, P("blk", "head")),
        check_vma=False,
    )
```

```python
import jax
import jax.numpy as jnp
from jax import lax
from jax.experimental import pallas as pl
from jax.experimental.pallas import tpu as pltpu
from jax.sharding import PartitionSpec as P

F32 = jnp.float32
BF16 = jnp.bfloat16
MESH = pl.DeviceIdType.MESH
SPAN = 512
TILE = 128
HEADS = 5
HALF = 320
COLS = 640
N_BLK = 64
SCALE = 128 ** -0.5
FAR = 1e30
ORDER = (2, 1, 3, 0)


def push(src, dst, send, recv, **where):
    return pltpu.make_async_remote_copy(
        src_ref=src,
        dst_ref=dst,
        send_sem=send,
        recv_sem=recv,
        device_id=where,
        device_id_type=MESH,
    )


def meet(peers):
    barrier = pltpu.get_barrier_semaphore()
    for where in peers:
        pl.semaphore_signal(barrier, inc=1, device_id=where, device_id_type=MESH)
    pl.semaphore_wait(barrier, len(peers))


def rows(start):
    return pl.ds(pl.multiple_of(start, TILE), TILE)


def around(y):
    return lax.rem(y + 1, 4), lax.rem(y + 3, 4), lax.rem(y + 2, 4)


def dot(a, b, contract):
    return lax.dot_general(a, b, (contract, ((), ())), preferred_element_type=F32)


def kernel(
    q_in, g_in, k_in, v_in, lse_in, a_hbm, l_hbm, listed, query_out, key_out, weight,
    a_in, l_in, lt, stat_in, far,
    win, kv, stat, entry_relay, gathered, dq, dk, dv, values, dq_out, dq_in, back, relay,
    x2_out, x2_in, xr_out, xr_in, xl_out, xl_in, total, z_out, z_in,
    y_send, y_recv, s_send, s_recv, h_send, h_recv, t_send, t_recv, l_send, l_recv,
    own_sem, g_send, g_recv, v_send, v_recv, q_send, q_recv,
    x_send, x_recv, z_send, z_recv, b_send, b_recv,
):
    b = lax.axis_index("blk")
    y = lax.axis_index("head")
    yr, yl, y2 = around(y)
    br, bl = lax.rem(b + 1, N_BLK), lax.rem(b + N_BLK - 1, N_BLK)
    core = lax.rem(b, 2)
    mate = b + 1 - 2 * core
    x = lax.rem(b // 2, 4)
    z = b // 8
    xr = z * 8 + lax.rem(x + 1, 4) * 2 + core
    xl = z * 8 + lax.rem(x + 3, 4) * 2 + core

    def pair(owner):
        return pl.ds(pl.multiple_of(owner * 256, 256), 256)

    lane = pl.ds(pl.multiple_of(y * 256 + core * 128, 128), 128)
    grads = (query_out, key_out)
    a_load = pltpu.make_async_copy(a_hbm, a_in, own_sem.at[0])
    l_load = pltpu.make_async_copy(l_hbm, l_in, own_sem.at[1])
    a_load.start()
    l_load.start()
    meet(
        [{"blk": b, "head": yr}, {"blk": b, "head": yl}, {"blk": b, "head": y2}]
        + [{"blk": br, "head": y}, {"blk": bl, "head": y}]
        + [{"blk": xr, "head": y}, {"blk": xl, "head": y}]
        + [{"blk": lax.rem(b + 8 * r, N_BLK), "head": y} for r in range(1, 8)]
    )

    def mine(ref, to):
        return ref.at[pl.ds(to * HEADS, HEADS)]

    def first(phase, srcs, dst, base):
        at = rows(base + y * TILE)
        plan = [
            (yr, mine(srcs[0], y2), entry_relay.at[phase, 0]),
            (yl, mine(srcs[1], y2), entry_relay.at[phase, 1]),
        ]
        for t in range(2):
            for where in (yr, yl):
                plan.append((where, mine(srcs[t], where), dst.at[t, :, at]))
        sends = []
        for i, (where, copy_from, copy_to) in enumerate(plan):
            sends.append(
                push(copy_from, copy_to, y_send.at[phase, i], y_recv.at[phase, i], blk=b, head=where)
            )
            sends[-1].start()
        return sends

    def second(phase, sends, dst, base):
        for j, (where, owner) in enumerate(((yr, yl), (yl, yr))):
            sends[j].wait_recv()
            sends.append(
                push(
                    entry_relay.at[phase, j], dst.at[j, :, rows(base + owner * TILE)],
                    y_send.at[phase, 6 + j], y_recv.at[phase, 6 + j], blk=b, head=where,
                )
            )
            sends[-1].start()

    keys = first(0, (k_in, v_in), kv, 0)
    halo = []
    halo_stat = {}

    def pass_on(i, srcs, stat_src, owner):
        for j, (where, base, at) in enumerate(((br, 0, 0), (bl, 2 * SPAN, 8))):
            for t in range(2):
                halo.append(
                    push(
                        srcs[t], win.at[t, :, rows(base + owner * TILE)],
                        h_send.at[i, j, t], h_recv.at[i, j, t], blk=where, head=y,
                    )
                )
                halo[-1].start()
            if stat_src is not None:
                stat_on(i, j, where, stat_src, at + owner)

    def stat_on(i, j, where, stat_src, at):
        halo_stat[i, j] = push(
            stat_src, stat.at[at], t_send.at[i, j], t_recv.at[i, j], blk=where, head=y
        )
        halo_stat[i, j].start()

    def landed(owner):
        return [win.at[t, :, rows(SPAN + owner * TILE)] for t in range(2)]

    pass_on(0, [mine(q_in, y), mine(g_in, y)], None, y)
    for h in range(HEADS):
        for t, (near, key) in enumerate(((q_in, k_in), (g_in, v_in))):
            win[t, h, rows(SPAN + y * TILE)] = near[y * HEADS + h]
            kv[t, h, rows(y * TILE)] = key[y * HEADS + h]
    a_load.wait()

    def head_stat(h, carry):
        product = g_in[h].astype(F32) * a_in[h].astype(F32)
        delta = jnp.sum(product.T, axis=0, keepdims=True)
        lse = lse_in[pl.ds(h, 1), :]
        tile = jnp.concatenate([lse, delta, jnp.zeros((6, TILE), F32)], axis=0)
        stat_in[h // HEADS, lax.rem(h, HEADS)] = tile
        return carry

    lax.fori_loop(0, 4 * HEADS, head_stat, 0)
    second(0, keys, kv, 0)
    queries = first(1, (q_in, g_in), win, SPAN)
    stat[4 + y] = stat_in[y]
    stat_sends = []
    for i, where in enumerate((yr, yl, y2)):
        stat_sends.append(
            push(stat_in.at[where], stat.at[4 + y], s_send.at[i], s_recv.at[i], blk=b, head=where)
        )
        stat_sends[-1].start()
    for j, (where, at) in enumerate(((br, 0), (bl, 8))):
        stat_on(0, j, where, stat_in.at[y], at + y)

    l_load.wait()
    for j in range(40):
        lt[128 * j : 128 * j + 128] = l_in[:, 128 * j : 128 * j + 128].T

    def rows_of(dx, k, c):
        to = (lax.rem(z + 3 + k, 8) * 4 + lax.rem(x + dx, 4)) * 2 + c
        return pl.ds(pl.multiple_of(to * 80, 16), 80)

    for i, dx in enumerate(ORDER):
        for k in range(8):
            gathered[i, k, :, lane] = lt[rows_of(dx, k, core)]
    swaps = []
    for i, dx in enumerate(ORDER):
        for k in range(8):
            swaps.append(
                push(
                    lt.at[rows_of(dx, k, 1 - core)], gathered.at[i, k, :, lane],
                    l_send.at[i, k], l_recv.at[i, k], blk=mate, head=y,
                )
            )
            swaps[-1].start()
    for row in range(12):
        block = b * 4 + (row - 4)
        inside = (block >= 0) & (block < 4 * N_BLK)
        at = jnp.clip(block, 0, 4 * N_BLK - 1)
        entries = [listed[slot, at] for slot in range(8)]
        lines = []
        for k in range(4):
            found = entries[0] == b * 4 + k
            for entry in entries[1:]:
                found = found | (entry == b * 4 + k)
            gap = jnp.where(found & inside, jnp.float32(0.0), jnp.float32(FAR))
            lines.append(jnp.full((1, TILE), gap, F32))
        far[row] = jnp.concatenate(lines + lines, axis=0)

    pieces = ((0, 0), (0, 1), (1, 0), (2, 0), (3, 0), (1, 1), (2, 1), (3, 1))
    gathers = {}

    def spread(p):
        i, half = pieces[p]
        if p in (0, 2, 3, 4):
            for copy in swaps[8 * i : 8 * i + 8]:
                copy.wait_recv()
        for j, where in enumerate((yr, yl)):
            piece = gathered.at[i, pl.ds(4 * half, 4), :, pair(y)]
            gathers[p, j] = push(
                piece, piece, g_send.at[p, j], g_recv.at[p, j], blk=b, head=where
            )
            gathers[p, j].start()

    def forward(p):
        i, half = pieces[p]
        for j, (where, owner) in enumerate(((yr, yl), (yl, yr))):
            gathers[p, j].wait_recv()
            piece = gathered.at[i, pl.ds(4 * half + 2 * j, 2), :, pair(owner)]
            gathers[p, 2 + j] = push(
                piece, piece, g_send.at[p, 2 + j], g_recv.at[p, 2 + j], blk=b, head=where
            )
            gathers[p, 2 + j].start()

    def product(p):
        i, half = pieces[p]
        gathers[p, 2].wait_recv()
        gathers[p, 3].wait_recv()
        left = gathered[i, 4 * half : 4 * half + 4].reshape(HALF, 1024)
        return dot(left, values[...].reshape(1024, COLS), ((1,), (0,)))

    def attend(owner, lead):
        spans = [rows(part * SPAN + owner * TILE) for part in range(3)]

        def one_head(h, carry):
            key, val = kv[0, h], kv[1, h]
            query = jnp.concatenate([win[0, h, at] for at in spans], axis=0)
            grad = jnp.concatenate([win[1, h, at] for at in spans], axis=0)
            tiles = [stat[4 * part + owner, h] for part in range(3)]
            lse = jnp.concatenate([tile[0:1] for tile in tiles], axis=1)
            delta = jnp.concatenate([tile[1:2] for tile in tiles], axis=1)
            apart = jnp.concatenate([far[4 * part + owner, 0:4] for part in range(3)], axis=1) + lse
            scores = dot(key, query, ((1,), (1,))) * SCALE
            dweights = dot(val, grad, ((1,), (1,)))
            weights = jnp.concatenate(
                [
                    jnp.exp(scores[k * TILE : (k + 1) * TILE] - apart[k : k + 1])
                    for k in range(4)
                ],
                axis=0,
            )
            dscores = (weights * (dweights - delta)).astype(BF16)
            weights = weights.astype(BF16)
            value_part = dot(weights, grad, ((1,), (0,)))
            key_part = dot(dscores, query, ((1,), (0,)))
            query_part = dot(dscores, key, ((0,), (0,))) * SCALE
            dq_out[0, h, rows(owner * TILE)] = query_part[:TILE].astype(BF16)
            dq[h, rows(owner * TILE)] = query_part[TILE : 2 * TILE]
            dq_out[1, h, rows(owner * TILE)] = query_part[2 * TILE :].astype(BF16)
            if lead:
                dv[h] = value_part
                dk[h] = key_part
            else:
                dv[h] += value_part
                dk[h] += key_part
            return carry

        lax.fori_loop(0, HEADS, one_head, 0)

    dq_copies = []

    def send_dq(i, owner):
        for j, where in enumerate((bl, br)):
            piece = (j, slice(None), rows(owner * TILE))
            dq_copies.append(
                push(
                    dq_out.at[piece], dq_in.at[piece],
                    q_send.at[i, j], q_recv.at[i, j], blk=where, head=y,
                )
            )
            dq_copies[-1].start()

    def halo_in(i):
        for copy in halo[4 * i : 4 * i + 4] + [halo_stat[i, 0], halo_stat[i, 1]]:
            copy.wait_recv()

    for copy in keys[2:]:
        copy.wait_recv()
    second(1, queries, win, SPAN)
    spread(0)
    spread(1)
    spread(2)
    halo_in(0)
    attend(y, True)
    for i, owner in ((0, yl), (1, yr)):
        queries[2 + i].wait_recv()
        queries[4 + i].wait_recv()
        stat_sends[i].wait_recv()
        pass_on(1 + i, landed(owner), stat.at[4 + owner], owner)
    queries[6].wait_recv()
    queries[7].wait_recv()
    stat_sends[2].wait_recv()
    pass_on(3, landed(y2), stat.at[4 + y2], y2)
    send_dq(0, y)
    halo_in(1)
    attend(yl, False)
    send_dq(1, yl)
    forward(0)
    halo_in(2)
    attend(yr, False)
    send_dq(2, yr)
    forward(1)
    spread(3)
    halo_in(3)
    attend(y2, False)

    for h in range(HEADS):
        cols = pl.ds(h * 128, 128)
        for k in range(4):
            values[k, core, :, cols] = dv[h, k * TILE : (k + 1) * TILE].astype(BF16)
    value_copy = push(
        values.at[:, core], values.at[:, core], v_send, v_recv, blk=mate, head=y
    )
    value_copy.start()
    forward(2)
    spread(4)
    value_copy.wait_recv()
    x_copies = {}

    def x_push(name, i, q, src, dst, where):
        copy = push(src.at[q], dst.at[q], x_send.at[i, q], x_recv.at[i, q], blk=where, head=y)
        copy.start()
        x_copies[name, q] = copy

    def quarters(value):
        return ((0, value[:160]), (1, value[160:]))

    for q, part in quarters(product(0)):
        x2_out[q] = part.astype(BF16)
        x_push("far", 0, q, x2_out, x2_in, xr)
    for q, part in quarters(product(1)):
        x2_out[2 + q] = part.astype(BF16)
        x_push("far", 0, 2 + q, x2_out, x2_in, xl)
    send_dq(3, y2)
    forward(3)
    spread(5)
    for h in range(HEADS):
        back[1, h] = (dk[h] * SCALE).astype(BF16)
    forward(4)
    spread(6)
    for q, part in quarters(product(2)):
        x_copies["far", q].wait_recv()
        xr_out[q] = (part + x2_in[q].astype(F32)).astype(BF16)
        x_push("right", 1, q, xr_out, xr_in, xr)
    for q, part in quarters(product(3)):
        xl_out[q] = part.astype(BF16)
        x_push("left", 2, q, xl_out, xl_in, xl)
    forward(5)
    spread(7)
    total[0:HALF] = product(4)
    for q, part in quarters(product(5)):
        xr_out[2 + q] = part.astype(BF16)
        x_push("right", 1, 2 + q, xr_out, xr_in, xr)
    forward(6)
    for q, part in quarters(product(6)):
        x_copies["far", 2 + q].wait_recv()
        xl_out[2 + q] = (part + x2_in[2 + q].astype(F32)).astype(BF16)
        x_push("left", 2, 2 + q, xl_out, xl_in, xl)
    forward(7)

    for copy in dq_copies:
        copy.wait_recv()
    for h in range(HEADS):
        back[0, h] = (
            dq[h] + dq_in[0, h].astype(F32) + dq_in[1, h].astype(F32)
        ).astype(BF16)
    plan = [
        (yr, back.at[0, :, rows(y2 * TILE)], relay.at[0]),
        (yl, back.at[1, :, rows(y2 * TILE)], relay.at[1]),
    ]
    for t in range(2):
        for where in (yr, yl):
            plan.append((where, back.at[t, :, rows(where * TILE)], mine(grads[t], y)))
    back_copies = []
    for i, (where, copy_from, copy_to) in enumerate(plan):
        back_copies.append(
            push(copy_from, copy_to, b_send.at[i], b_recv.at[i], blk=b, head=where)
        )
        back_copies[-1].start()
    for t in range(2):
        for h in range(HEADS):
            grads[t][y * HEADS + h] = back[t, h, rows(y * TILE)]

    z_copies = {}

    def reduce_quarter(q):
        x_copies["right", q].wait_recv()
        x_copies["left", q].wait_recv()
        at = pl.ds(160 * q, 160)
        summed = total[at] + xr_in[q].astype(F32) + xl_in[q].astype(F32)
        for k in range(2):
            r = (3 + 2 * q + k) % 8
            part = summed[80 * k : 80 * k + 80]
            if r == 0:
                weight[...] = part
                continue
            z_out[r] = part.astype(BF16)
            z_copies[r] = push(
                z_out.at[r], z_in.at[r], z_send.at[r], z_recv.at[r],
                blk=lax.rem(b + 8 * r, N_BLK), head=y,
            )
            z_copies[r].start()

    reduce_quarter(0)
    reduce_quarter(1)
    total[HALF : 2 * HALF] = product(7)
    reduce_quarter(2)
    for j, (where, owner) in enumerate(((yr, yl), (yl, yr))):
        back_copies[j].wait_recv()
        back_copies.append(
            push(
                relay.at[j], mine(grads[j], owner),
                b_send.at[6 + j], b_recv.at[6 + j], blk=b, head=where,
            )
        )
        back_copies[-1].start()

    reduce_quarter(3)
    result = weight[...]
    for r in (3, 4, 5, 6, 7, 1, 2):
        z_copies[r].wait_recv()
        result = result + z_in[r].astype(F32)
    weight[...] = result
    for copy in back_copies[2:]:
        copy.wait_recv()
    copies = queries + keys + stat_sends + halo + swaps + list(gathers.values())
    copies += list(x_copies.values()) + list(z_copies.values()) + list(halo_stat.values())
    for copy in copies + [value_copy] + dq_copies + back_copies:
        copy.wait_send()


VMEM_SPEC = pl.BlockSpec(memory_space=pltpu.VMEM)
ANY_SPEC = pl.BlockSpec(memory_space=pl.ANY)


def sems(*shape):
    return pltpu.SemaphoreType.DMA(shape) if shape else pltpu.SemaphoreType.DMA


def local(
    layer_input, queries, key_vectors, value_vectors, out_grad, attn_out, log_sum, block_list
):
    by_head = [
        jnp.swapaxes(array, 0, 1)
        for array in (queries, out_grad, key_vectors, value_vectors, attn_out)
    ]
    query_grad, key_grad, weight_grad = pl.pallas_call(
        kernel,
        out_shape=(
            jax.ShapeDtypeStruct((20, TILE, 128), BF16),
            jax.ShapeDtypeStruct((20, TILE, 128), BF16),
            jax.ShapeDtypeStruct((80, COLS), F32),
        ),
        in_specs=[VMEM_SPEC] * 5 + [ANY_SPEC] * 2 + [pl.BlockSpec(memory_space=pltpu.SMEM)],
        out_specs=[VMEM_SPEC] * 3,
        scratch_shapes=[
            pltpu.VMEM((20, TILE, 128), BF16),
            pltpu.VMEM((TILE, 5120), BF16),
            pltpu.VMEM((5120, TILE), BF16),
            pltpu.VMEM((4, HEADS, 8, TILE), F32),
            pltpu.VMEM((12, 8, TILE), F32),
            pltpu.VMEM((2, HEADS, 3 * SPAN, 128), BF16),
            pltpu.VMEM((2, HEADS, SPAN, 128), BF16),
            pltpu.VMEM((12, HEADS, 8, TILE), F32),
            pltpu.VMEM((2, 2, HEADS, TILE, 128), BF16),
            pltpu.VMEM((4, 8, 80, 1024), BF16),
            pltpu.VMEM((HEADS, SPAN, 128), F32),
            pltpu.VMEM((HEADS, SPAN, 128), F32),
            pltpu.VMEM((HEADS, SPAN, 128), F32),
            pltpu.VMEM((4, 2, TILE, COLS), BF16),
            pltpu.VMEM((2, HEADS, SPAN, 128), BF16),
            pltpu.VMEM((2, HEADS, SPAN, 128), BF16),
            pltpu.VMEM((2, HEADS, SPAN, 128), BF16),
            pltpu.VMEM((2, HEADS, TILE, 128), BF16),
        ]
        + [pltpu.VMEM((4, 160, COLS), BF16)] * 6
        + [
            pltpu.VMEM((2 * HALF, COLS), F32),
            pltpu.VMEM((8, 80, COLS), BF16),
            pltpu.VMEM((8, 80, COLS), BF16),
            sems(2, 8), sems(2, 8), sems(3), sems(3), sems(4, 2, 2), sems(4, 2, 2),
            sems(4, 2), sems(4, 2), sems(4, 8), sems(4, 8),
            sems(2), sems(8, 4), sems(8, 4), sems(), sems(), sems(4, 2), sems(4, 2),
            sems(3, 4), sems(3, 4), sems(8), sems(8), sems(8), sems(8),
        ],
        compiler_params=pltpu.CompilerParams(
            collective_id=0, has_side_effects=True, vmem_limit_bytes=60 * 2**20
        ),
        name="layer",
    )(*by_head[:4], log_sum.T, by_head[4], layer_input, block_list.T)
    return (jnp.swapaxes(query_grad, 0, 1), jnp.swapaxes(key_grad, 0, 1), weight_grad)


def solution(mesh):
    both = ("blk", "head")
    rows3 = P(both, None, None)
    return jax.shard_map(
        local,
        mesh=mesh,
        in_specs=(P(both, None),) + (rows3,) * 5 + (P(both, None), P()),
        out_specs=(rows3, rows3, P("blk", "head")),
        check_vma=False,
    )
```

```python
import jax
import jax.numpy as jnp
from jax import lax
from jax.experimental import pallas as pl
from jax.experimental.pallas import tpu as pltpu
from jax.sharding import PartitionSpec as P

F32 = jnp.float32
BF16 = jnp.bfloat16
MESH = pl.DeviceIdType.MESH
SPAN = 512
TILE = 128
HEADS = 5
HALF = 320
COLS = 640
N_BLK = 64
SCALE = 128 ** -0.5
FAR = 1e30
ORDER = (2, 1, 3, 0)


def push(src, dst, send, recv, **where):
    return pltpu.make_async_remote_copy(
        src_ref=src,
        dst_ref=dst,
        send_sem=send,
        recv_sem=recv,
        device_id=where,
        device_id_type=MESH,
    )


def meet(peers):
    barrier = pltpu.get_barrier_semaphore()
    for where in peers:
        pl.semaphore_signal(barrier, inc=1, device_id=where, device_id_type=MESH)
    pl.semaphore_wait(barrier, len(peers))


def rows(start):
    return pl.ds(pl.multiple_of(start, TILE), TILE)


def around(y):
    return lax.rem(y + 1, 4), lax.rem(y + 3, 4), lax.rem(y + 2, 4)


def dot(a, b, contract):
    return lax.dot_general(a, b, (contract, ((), ())), preferred_element_type=F32)


def kernel(
    q_hbm, g_hbm, k_in, v_in, lse_in, a_hbm, l_hbm, listed, query_out, key_out, weight,
    q_in, g_in, a_in, l_in, lt, stat_in, far,
    win, kv, stat, entry_relay, gathered, dq, dk, dv, values, dq_out, dq_in, back, relay,
    x2_out, x2_in, xr_out, xr_in, xl_out, xl_in, total, z_out, z_in,
    y_send, y_recv, s_send, s_recv, h_send, h_recv, t_send, t_recv, l_send, l_recv,
    own_sem, g_send, g_recv, v_send, v_recv, q_send, q_recv,
    x_send, x_recv, z_send, z_recv, b_send, b_recv,
):
    b = lax.axis_index("blk")
    y = lax.axis_index("head")
    yr, yl, y2 = around(y)
    br, bl = lax.rem(b + 1, N_BLK), lax.rem(b + N_BLK - 1, N_BLK)
    core = lax.rem(b, 2)
    mate = b + 1 - 2 * core
    x = lax.rem(b // 2, 4)
    z = b // 8
    xr = z * 8 + lax.rem(x + 1, 4) * 2 + core
    xl = z * 8 + lax.rem(x + 3, 4) * 2 + core

    def pair(owner):
        return pl.ds(pl.multiple_of(owner * 256, 256), 256)

    lane = pl.ds(pl.multiple_of(y * 256 + core * 128, 128), 128)
    grads = (query_out, key_out)
    q_load = pltpu.make_async_copy(q_hbm, q_in, own_sem.at[2])
    g_load = pltpu.make_async_copy(g_hbm, g_in, own_sem.at[3])
    q_load.start()
    g_load.start()
    a_load = pltpu.make_async_copy(a_hbm, a_in, own_sem.at[0])
    l_load = pltpu.make_async_copy(l_hbm, l_in, own_sem.at[1])
    a_load.start()
    l_load.start()
    meet(
        [{"blk": b, "head": yr}, {"blk": b, "head": yl}, {"blk": b, "head": y2}]
        + [{"blk": br, "head": y}, {"blk": bl, "head": y}]
        + [{"blk": xr, "head": y}, {"blk": xl, "head": y}]
        + [{"blk": lax.rem(b + 8 * r, N_BLK), "head": y} for r in range(1, 8)]
    )

    def mine(ref, to):
        return ref.at[pl.ds(to * HEADS, HEADS)]

    def first(phase, srcs, dst, base):
        at = rows(base + y * TILE)
        plan = [
            (yr, mine(srcs[0], y2), entry_relay.at[phase, 0]),
            (yl, mine(srcs[1], y2), entry_relay.at[phase, 1]),
        ]
        for t in range(2):
            for where in (yr, yl):
                plan.append((where, mine(srcs[t], where), dst.at[t, :, at]))
        sends = []
        for i, (where, copy_from, copy_to) in enumerate(plan):
            sends.append(
                push(copy_from, copy_to, y_send.at[phase, i], y_recv.at[phase, i], blk=b, head=where)
            )
            sends[-1].start()
        return sends

    def second(phase, sends, dst, base):
        for j, (where, owner) in enumerate(((yr, yl), (yl, yr))):
            sends[j].wait_recv()
            sends.append(
                push(
                    entry_relay.at[phase, j], dst.at[j, :, rows(base + owner * TILE)],
                    y_send.at[phase, 6 + j], y_recv.at[phase, 6 + j], blk=b, head=where,
                )
            )
            sends[-1].start()

    keys = first(0, (k_in, v_in), kv, 0)
    halo = []
    halo_stat = {}

    def pass_on(i, srcs, stat_src, owner):
        for j, (where, base, at) in enumerate(((br, 0, 0), (bl, 2 * SPAN, 8))):
            for t in range(2):
                halo.append(
                    push(
                        srcs[t], win.at[t, :, rows(base + owner * TILE)],
                        h_send.at[i, j, t], h_recv.at[i, j, t], blk=where, head=y,
                    )
                )
                halo[-1].start()
            if stat_src is not None:
                stat_on(i, j, where, stat_src, at + owner)

    def stat_on(i, j, where, stat_src, at):
        halo_stat[i, j] = push(
            stat_src, stat.at[at], t_send.at[i, j], t_recv.at[i, j], blk=where, head=y
        )
        halo_stat[i, j].start()

    def landed(owner):
        return [win.at[t, :, rows(SPAN + owner * TILE)] for t in range(2)]

    q_load.wait()
    g_load.wait()
    pass_on(0, [mine(q_in, y), mine(g_in, y)], None, y)
    for h in range(HEADS):
        for t, (near, key) in enumerate(((q_in, k_in), (g_in, v_in))):
            win[t, h, rows(SPAN + y * TILE)] = near[y * HEADS + h]
            kv[t, h, rows(y * TILE)] = key[y * HEADS + h]
    a_load.wait()

    def head_stat(h, carry):
        product = g_in[h].astype(F32) * a_in[h].astype(F32)
        delta = jnp.sum(product.T, axis=0, keepdims=True)
        lse = lse_in[pl.ds(h, 1), :]
        tile = jnp.concatenate([lse, delta, jnp.zeros((6, TILE), F32)], axis=0)
        stat_in[h // HEADS, lax.rem(h, HEADS)] = tile
        return carry

    lax.fori_loop(0, 4 * HEADS, head_stat, 0)
    second(0, keys, kv, 0)
    queries = first(1, (q_in, g_in), win, SPAN)
    stat[4 + y] = stat_in[y]
    stat_sends = []
    for i, where in enumerate((yr, yl, y2)):
        stat_sends.append(
            push(stat_in.at[where], stat.at[4 + y], s_send.at[i], s_recv.at[i], blk=b, head=where)
        )
        stat_sends[-1].start()
    for j, (where, at) in enumerate(((br, 0), (bl, 8))):
        stat_on(0, j, where, stat_in.at[y], at + y)

    l_load.wait()
    for j in range(40):
        lt[128 * j : 128 * j + 128] = l_in[:, 128 * j : 128 * j + 128].T

    def rows_of(dx, k, c):
        to = (lax.rem(z + 3 + k, 8) * 4 + lax.rem(x + dx, 4)) * 2 + c
        return pl.ds(pl.multiple_of(to * 80, 16), 80)

    for i, dx in enumerate(ORDER):
        for k in range(8):
            gathered[i, k, :, lane] = lt[rows_of(dx, k, core)]
    swaps = []
    for i, dx in enumerate(ORDER):
        for k in range(8):
            swaps.append(
                push(
                    lt.at[rows_of(dx, k, 1 - core)], gathered.at[i, k, :, lane],
                    l_send.at[i, k], l_recv.at[i, k], blk=mate, head=y,
                )
            )
            swaps[-1].start()
    for row in range(12):
        block = b * 4 + (row - 4)
        inside = (block >= 0) & (block < 4 * N_BLK)
        at = jnp.clip(block, 0, 4 * N_BLK - 1)
        entries = [listed[slot, at] for slot in range(8)]
        lines = []
        for k in range(4):
            found = entries[0] == b * 4 + k
            for entry in entries[1:]:
                found = found | (entry == b * 4 + k)
            gap = jnp.where(found & inside, jnp.float32(0.0), jnp.float32(FAR))
            lines.append(jnp.full((1, TILE), gap, F32))
        far[row] = jnp.concatenate(lines + lines, axis=0)

    pieces = ((0, 0), (0, 1), (1, 0), (2, 0), (3, 0), (1, 1), (2, 1), (3, 1))
    gathers = {}

    def spread(p):
        i, half = pieces[p]
        if p in (0, 2, 3, 4):
            for copy in swaps[8 * i : 8 * i + 8]:
                copy.wait_recv()
        for j, where in enumerate((yr, yl)):
            piece = gathered.at[i, pl.ds(4 * half, 4), :, pair(y)]
            gathers[p, j] = push(
                piece, piece, g_send.at[p, j], g_recv.at[p, j], blk=b, head=where
            )
            gathers[p, j].start()

    def forward(p):
        i, half = pieces[p]
        for j, (where, owner) in enumerate(((yr, yl), (yl, yr))):
            gathers[p, j].wait_recv()
            piece = gathered.at[i, pl.ds(4 * half + 2 * j, 2), :, pair(owner)]
            gathers[p, 2 + j] = push(
                piece, piece, g_send.at[p, 2 + j], g_recv.at[p, 2 + j], blk=b, head=where
            )
            gathers[p, 2 + j].start()

    def product(p):
        i, half = pieces[p]
        gathers[p, 2].wait_recv()
        gathers[p, 3].wait_recv()
        left = gathered[i, 4 * half : 4 * half + 4].reshape(HALF, 1024)
        return dot(left, values[...].reshape(1024, COLS), ((1,), (0,)))

    def attend(tiles_of, lead):
        spans = [rows(part * SPAN + owner * TILE) for part, owner in tiles_of]

        def one_head(h, carry):
            key, val = kv[0, h], kv[1, h]
            query = jnp.concatenate([win[0, h, at] for at in spans], axis=0)
            grad = jnp.concatenate([win[1, h, at] for at in spans], axis=0)
            tiles = [stat[4 * part + owner, h] for part, owner in tiles_of]
            lse = jnp.concatenate([tile[0:1] for tile in tiles], axis=1)
            delta = jnp.concatenate([tile[1:2] for tile in tiles], axis=1)
            apart = jnp.concatenate([far[4 * part + owner, 0:4] for part, owner in tiles_of], axis=1) + lse
            scores = dot(key, query, ((1,), (1,))) * SCALE
            dweights = dot(val, grad, ((1,), (1,)))
            weights = jnp.concatenate(
                [
                    jnp.exp(scores[k * TILE : (k + 1) * TILE] - apart[k : k + 1])
                    for k in range(4)
                ],
                axis=0,
            )
            dscores = (weights * (dweights - delta)).astype(BF16)
            weights = weights.astype(BF16)
            value_part = dot(weights, grad, ((1,), (0,)))
            key_part = dot(dscores, query, ((1,), (0,)))
            query_part = dot(dscores, key, ((0,), (0,))) * SCALE
            for n, (part, owner) in enumerate(tiles_of):
                piece = query_part[n * TILE : (n + 1) * TILE]
                if part == 1:
                    dq[h, rows(owner * TILE)] = piece
                else:
                    dq_out[part // 2, h, rows(owner * TILE)] = piece.astype(BF16)
            if lead:
                dv[h] = value_part
                dk[h] = key_part
            else:
                dv[h] += value_part
                dk[h] += key_part
            return carry

        lax.fori_loop(0, HEADS, one_head, 0)

    dq_copies = []

    def send_dq(i, owner):
        for j, where in enumerate((bl, br)):
            piece = (j, slice(None), rows(owner * TILE))
            dq_copies.append(
                push(
                    dq_out.at[piece], dq_in.at[piece],
                    q_send.at[i, j], q_recv.at[i, j], blk=where, head=y,
                )
            )
            dq_copies[-1].start()

    def halo_in(i):
        for copy in halo[4 * i : 4 * i + 4] + [halo_stat[i, 0], halo_stat[i, 1]]:
            copy.wait_recv()

    for copy in keys[2:]:
        copy.wait_recv()
    second(1, queries, win, SPAN)
    spread(0)
    spread(1)
    spread(2)
    halo_in(0)
    attend([(0, y), (1, y), (2, y)], True)
    for i, owner in ((0, yl), (1, yr)):
        queries[2 + i].wait_recv()
        queries[4 + i].wait_recv()
        stat_sends[i].wait_recv()
        pass_on(1 + i, landed(owner), stat.at[4 + owner], owner)
    attend([(1, yl), (1, yr)], False)
    queries[6].wait_recv()
    queries[7].wait_recv()
    stat_sends[2].wait_recv()
    pass_on(3, landed(y2), stat.at[4 + y2], y2)
    send_dq(0, y)
    halo_in(1)
    attend([(0, yl), (2, yl), (1, y2)], False)
    send_dq(1, yl)
    forward(0)
    halo_in(2)
    attend([(0, yr), (2, yr)], False)
    send_dq(2, yr)
    forward(1)
    spread(3)
    halo_in(3)
    attend([(0, y2), (2, y2)], False)

    for h in range(HEADS):
        cols = pl.ds(h * 128, 128)
        for k in range(4):
            values[k, core, :, cols] = dv[h, k * TILE : (k + 1) * TILE].astype(BF16)
    value_copy = push(
        values.at[:, core], values.at[:, core], v_send, v_recv, blk=mate, head=y
    )
    value_copy.start()
    forward(2)
    spread(4)
    value_copy.wait_recv()
    plan = [
        (yr, back.at[0, :, rows(y2 * TILE)], relay.at[0]),
        (yl, back.at[1, :, rows(y2 * TILE)], relay.at[1]),
    ]
    for t in range(2):
        for where in (yr, yl):
            plan.append((where, back.at[t, :, rows(where * TILE)], mine(grads[t], y)))
    back_copies = {}

    def send_back(i):
        where, copy_from, copy_to = plan[i]
        back_copies[i] = push(copy_from, copy_to, b_send.at[i], b_recv.at[i], blk=b, head=where)
        back_copies[i].start()

    x_copies = {}

    def x_push(name, i, q, src, dst, where):
        copy = push(src.at[q], dst.at[q], x_send.at[i, q], x_recv.at[i, q], blk=where, head=y)
        copy.start()
        x_copies[name, q] = copy

    def quarters(value):
        return ((0, value[:160]), (1, value[160:]))

    for q, part in quarters(product(0)):
        x2_out[q] = part.astype(BF16)
        x_push("far", 0, q, x2_out, x2_in, xr)
    for q, part in quarters(product(1)):
        x2_out[2 + q] = part.astype(BF16)
        x_push("far", 0, 2 + q, x2_out, x2_in, xl)
    send_dq(3, y2)
    forward(3)
    spread(5)
    for h in range(HEADS):
        back[1, h] = (dk[h] * SCALE).astype(BF16)
    forward(4)
    spread(6)
    for q, part in quarters(product(2)):
        x_copies["far", q].wait_recv()
        xr_out[q] = (part + x2_in[q].astype(F32)).astype(BF16)
        x_push("right", 1, q, xr_out, xr_in, xr)
    for q, part in quarters(product(3)):
        xl_out[q] = part.astype(BF16)
        x_push("left", 2, q, xl_out, xl_in, xl)
    forward(5)
    spread(7)
    total[0:HALF] = product(4)
    for q, part in quarters(product(5)):
        xr_out[2 + q] = part.astype(BF16)
        x_push("right", 1, 2 + q, xr_out, xr_in, xr)
    forward(6)
    for q, part in quarters(product(6)):
        x_copies["far", 2 + q].wait_recv()
        xl_out[2 + q] = (part + x2_in[2 + q].astype(F32)).astype(BF16)
        x_push("left", 2, 2 + q, xl_out, xl_in, xl)
    for i in (1, 4, 5):
        send_back(i)
    forward(7)

    for copy in dq_copies:
        copy.wait_recv()
    for h in range(HEADS):
        back[0, h] = (
            dq[h] + dq_in[0, h].astype(F32) + dq_in[1, h].astype(F32)
        ).astype(BF16)
    for i in (0, 2, 3):
        send_back(i)
    for t in range(2):
        for h in range(HEADS):
            grads[t][y * HEADS + h] = back[t, h, rows(y * TILE)]

    z_copies = {}

    def reduce_quarter(q):
        x_copies["right", q].wait_recv()
        x_copies["left", q].wait_recv()
        at = pl.ds(160 * q, 160)
        summed = total[at] + xr_in[q].astype(F32) + xl_in[q].astype(F32)
        for k in range(2):
            r = (3 + 2 * q + k) % 8
            part = summed[80 * k : 80 * k + 80]
            if r == 0:
                weight[...] = part
                continue
            z_out[r] = part.astype(BF16)
            z_copies[r] = push(
                z_out.at[r], z_in.at[r], z_send.at[r], z_recv.at[r],
                blk=lax.rem(b + 8 * r, N_BLK), head=y,
            )
            z_copies[r].start()

    reduce_quarter(0)
    reduce_quarter(1)
    total[HALF : 2 * HALF] = product(7)
    reduce_quarter(2)
    for j, (where, owner) in enumerate(((yr, yl), (yl, yr))):
        back_copies[j].wait_recv()
        back_copies[6 + j] = push(
            relay.at[j], mine(grads[j], owner),
            b_send.at[6 + j], b_recv.at[6 + j], blk=b, head=where,
        )
        back_copies[6 + j].start()
    reduce_quarter(3)
    result = weight[...]
    for r in (3, 4, 5, 6, 7, 1, 2):
        z_copies[r].wait_recv()
        result = result + z_in[r].astype(F32)
    weight[...] = result
    for i in range(2, 8):
        back_copies[i].wait_recv()
    copies = queries + keys + stat_sends + halo + swaps + list(gathers.values())
    copies += list(x_copies.values()) + list(z_copies.values()) + list(halo_stat.values())
    for copy in copies + [value_copy] + dq_copies + list(back_copies.values()):
        copy.wait_send()


VMEM_SPEC = pl.BlockSpec(memory_space=pltpu.VMEM)
ANY_SPEC = pl.BlockSpec(memory_space=pl.ANY)


def sems(*shape):
    return pltpu.SemaphoreType.DMA(shape) if shape else pltpu.SemaphoreType.DMA


def local(
    layer_input, queries, key_vectors, value_vectors, out_grad, attn_out, log_sum, block_list
):
    by_head = [
        jnp.swapaxes(array, 0, 1)
        for array in (queries, out_grad, key_vectors, value_vectors, attn_out)
    ]
    query_grad, key_grad, weight_grad = pl.pallas_call(
        kernel,
        out_shape=(
            jax.ShapeDtypeStruct((20, TILE, 128), BF16),
            jax.ShapeDtypeStruct((20, TILE, 128), BF16),
            jax.ShapeDtypeStruct((80, COLS), F32),
        ),
        in_specs=[ANY_SPEC] * 2 + [VMEM_SPEC] * 3 + [ANY_SPEC] * 2 + [pl.BlockSpec(memory_space=pltpu.SMEM)],
        out_specs=[VMEM_SPEC] * 3,
        scratch_shapes=[
            pltpu.VMEM((20, TILE, 128), BF16),
            pltpu.VMEM((20, TILE, 128), BF16),
            pltpu.VMEM((20, TILE, 128), BF16),
            pltpu.VMEM((TILE, 5120), BF16),
            pltpu.VMEM((5120, TILE), BF16),
            pltpu.VMEM((4, HEADS, 8, TILE), F32),
            pltpu.VMEM((12, 8, TILE), F32),
            pltpu.VMEM((2, HEADS, 3 * SPAN, 128), BF16),
            pltpu.VMEM((2, HEADS, SPAN, 128), BF16),
            pltpu.VMEM((12, HEADS, 8, TILE), F32),
            pltpu.VMEM((2, 2, HEADS, TILE, 128), BF16),
            pltpu.VMEM((4, 8, 80, 1024), BF16),
            pltpu.VMEM((HEADS, SPAN, 128), F32),
            pltpu.VMEM((HEADS, SPAN, 128), F32),
            pltpu.VMEM((HEADS, SPAN, 128), F32),
            pltpu.VMEM((4, 2, TILE, COLS), BF16),
            pltpu.VMEM((2, HEADS, SPAN, 128), BF16),
            pltpu.VMEM((2, HEADS, SPAN, 128), BF16),
            pltpu.VMEM((2, HEADS, SPAN, 128), BF16),
            pltpu.VMEM((2, HEADS, TILE, 128), BF16),
        ]
        + [pltpu.VMEM((4, 160, COLS), BF16)] * 6
        + [
            pltpu.VMEM((2 * HALF, COLS), F32),
            pltpu.VMEM((8, 80, COLS), BF16),
            pltpu.VMEM((8, 80, COLS), BF16),
            sems(2, 8), sems(2, 8), sems(3), sems(3), sems(4, 2, 2), sems(4, 2, 2),
            sems(4, 2), sems(4, 2), sems(4, 8), sems(4, 8),
            sems(4), sems(8, 4), sems(8, 4), sems(), sems(), sems(4, 2), sems(4, 2),
            sems(3, 4), sems(3, 4), sems(8), sems(8), sems(8), sems(8),
        ],
        compiler_params=pltpu.CompilerParams(
            collective_id=0, has_side_effects=True, vmem_limit_bytes=60 * 2**20
        ),
        name="layer",
    )(*by_head[:4], log_sum.T, by_head[4], layer_input, block_list.T)
    return (jnp.swapaxes(query_grad, 0, 1), jnp.swapaxes(key_grad, 0, 1), weight_grad)


def solution(mesh):
    both = ("blk", "head")
    rows3 = P(both, None, None)
    return jax.shard_map(
        local,
        mesh=mesh,
        in_specs=(P(both, None),) + (rows3,) * 5 + (P(both, None), P()),
        out_specs=(rows3, rows3, P("blk", "head")),
        check_vma=False,
    )
```
